256 devices in a mesh: sta: 16 (over x_hi, y, core), cel: 16 (over x_lo, z).
Axes of the slice: x: 4 (x_hi: 2, x_lo: 2; x = x_hi * 2 + x_lo), y: 4, z: 8, core: 2. Of those that a mesh axis runs over, the one named last changes fastest.
Arguments:
- station_plane: int32 [2, 65536], P(None, 'sta'), may hold values from 0 to 191
- station_height: int32 [65536], P('sta'), may hold values from 1 to 4
- cell_plane: int32 [2, 32768], P(None, 'cel'), may hold values from 0 to 191
- cell_depth: int32 [32768], P('cel'), may hold values from 0 to 15
- cell_density: float32 [32768], P('cel'), may hold values from 0.4 to 4
- left_before: float32 [16, 65536], P(None, 'sta'), may hold values from -6 to 6
- left_now: float32 [16, 65536], P(None, 'sta'), may hold values from -6 to 6
- right_before: float32 [16, 32768], P(None, 'cel'), may hold values from -6 to 6
Outputs:
- right_blocks: float32 [2, 16, 32768], P(None, None, 'cel')
- left_block: float32 [16, 65536], P(None, 'sta')
- alphas: float32 [2, 16, 16], replicated
- betas: float32 [2, 16, 16], replicated
The draws below stay inside these ranges and needn't reach their ends.
All inputs are finite; a program needn't handle non-finite values.
Results may differ from the reference program's by a relative error of at most 0.0003.
Values sent between devices are 32-bit elements; how exact they have to be, the bound alone decides.
No kernel may reach another device: no remote copies, remote signals or barrier semaphores. Data moves between devices by JAX's collectives and lax.ppermute only.
A program may use at most 64 MiB of HBM per device.

```python
import math
import jax
import jax.numpy as jnp
from jax import lax

RHS = 16
STEPS = 2
SPAN = 192
DEPTH = 16
STATIONS = 65536
CELLS = 32768


def set_ends(result, stream_key, least, top_value):
    longest = result.shape.index(max(result.shape))
    spots = []
    for shift in (0, 1):
        where = [jax.random.randint(jax.random.fold_in(stream_key, axis), (), 0, length) for axis, length in enumerate(result.shape)]
        where[longest] = (where[longest] + shift) % result.shape[longest]
        spots.append(tuple(where))
    return result.at[spots[0]].set(least).at[spots[1]].set(top_value)


def block_scale(rng, extent, cuts, smallest, largest):
    gain, own = 1.0, jax.random.fold_in(rng, 6)
    for position, blocks in cuts:
        heights = jnp.exp(jax.random.uniform(jax.random.fold_in(own, position), (blocks,), jnp.float32, smallest / len(cuts), largest / len(cuts)))
        gain = gain * jnp.repeat(heights, extent[position] // blocks).reshape([-1 if axis == position else 1 for axis in range(len(extent))])
    return gain


def scatter_about(rng, shape, spread, most, shards=(), dtype=jnp.bfloat16):
    array = jax.random.normal(rng, shape, jnp.float32) * spread
    if len(shards) > 0:
        array = block_scale(rng, shape, shards, -0.22, 0.18) * array
    return jnp.clip(array, min=-most, max=most).astype(dtype)


def setup_inputs(seed: int = 0) -> dict:
    key_list = jax.random.split(jax.random.key(seed), 9)
    station_plane = set_ends(jax.random.randint(key_list[0], (2, STATIONS), 0, SPAN), jax.random.fold_in(key_list[0], 1), 0, SPAN - 1).astype(jnp.int32)
    station_height = set_ends(jax.random.randint(key_list[1], (STATIONS,), 1, 5), jax.random.fold_in(key_list[1], 1), 1, 4).astype(jnp.int32)
    cell_plane = set_ends(jax.random.randint(key_list[2], (2, CELLS), 0, SPAN), jax.random.fold_in(key_list[2], 1), 0, SPAN - 1).astype(jnp.int32)
    cell_depth = set_ends(jax.random.randint(key_list[3], (CELLS,), 0, DEPTH), jax.random.fold_in(key_list[3], 1), 0, DEPTH - 1).astype(jnp.int32)
    cell_density = jnp.clip(jnp.exp(math.log(4.0) - 2.3025851 * jax.random.uniform(key_list[4], (CELLS,), jnp.float32) ** block_scale(key_list[4], (CELLS,), ((0, 16),), -0.2, 0.2)), 0.4, 4.0)
    left_before = scatter_about(key_list[5], (RHS, STATIONS), 1.0, 6.0, ((1, 16),), jnp.float32)
    left_now = scatter_about(key_list[6], (RHS, STATIONS), 1.0, 6.0, ((1, 16),), jnp.float32)
    right_before = scatter_about(key_list[7], (RHS, CELLS), 1.0, 6.0, ((1, 16),), jnp.float32)
    return {"station_plane": station_plane, "station_height": station_height, "cell_plane": cell_plane, "cell_depth": cell_depth, "cell_density": cell_density, "left_before": left_before, "left_now": left_now, "right_before": right_before}


GAIN = 4.0
HIGH = lax.Precision.HIGHEST

def kernel_rows(sx, sy, sz, cx, cy, cz, density):
    dx = sx[:, None] - cx[None, :]
    dy = sy[:, None] - cy[None, :]
    dz = sz[:, None] + cz[None, :] + 0.5
    square = dx * dx + dy * dy + dz * dz
    inverse = lax.rsqrt(square)
    inv_two = inverse * inverse
    return GAIN * density[None, :] * (2.0 * dz * dz - dx * dx - dy * dy) * (inv_two * inv_two * inverse)

def matmul(a, b):
    return jnp.dot(a.astype(jnp.float32), b.astype(jnp.float32), precision=HIGH, preferred_element_type=jnp.float32)

def orthonormal(block, basis, rows):
    coef = matmul(basis, block.T) / rows
    rest = block - matmul(coef.T, basis)
    gram = matmul(rest, rest.T) / rows
    lower = jnp.linalg.cholesky(gram)
    return (jax.scipy.linalg.solve_triangular(lower, rest, lower=True), lower)

def reference(station_plane, station_height, cell_plane, cell_depth, cell_density, left_before, left_now, right_before):
    sx = station_plane[0].astype(jnp.float32)
    sy = station_plane[1].astype(jnp.float32)
    sz = station_height.astype(jnp.float32)
    cx = cell_plane[0].astype(jnp.float32)
    cy = cell_plane[1].astype(jnp.float32)
    cz = cell_depth.astype(jnp.float32)
    block = 1024 if STATIONS % 1024 == 0 else STATIONS
    count = STATIONS // block
    sx_b = sx.reshape(count, block)
    sy_b = sy.reshape(count, block)
    sz_b = sz.reshape(count, block)

    def adjoint(left):
        left_b = left.reshape(RHS, count, block).transpose(1, 0, 2)

        def add_block(total, pieces):
            a, b, c, rows = pieces
            return (total + matmul(rows, kernel_rows(a, b, c, cx, cy, cz, cell_density)), None)
        total, unused = lax.scan(add_block, jnp.zeros((RHS, CELLS), jnp.float32), (sx_b, sy_b, sz_b, left_b))
        return total

    def forward(right):

        def one_block(pieces):
            a, b, c = pieces
            return matmul(right, kernel_rows(a, b, c, cx, cy, cz, cell_density).T)
        parts = lax.map(one_block, (sx_b, sy_b, sz_b))
        return parts.transpose(1, 0, 2).reshape(RHS, STATIONS)
    right_basis = right_before
    left_basis = jnp.concatenate([left_before, left_now], 0)
    left = left_now
    rights, alphas, betas = ([], [], [])
    for step in range(STEPS):
        right, alpha = orthonormal(adjoint(left), right_basis, CELLS)
        right_basis = jnp.concatenate([right_basis, right], 0)
        left, beta = orthonormal(forward(right), left_basis, STATIONS)
        left_basis = jnp.concatenate([left_basis, left], 0)
        rights.append(right)
        alphas.append(alpha)
        betas.append(beta)
    return (jnp.stack(rights), left, jnp.stack(alphas), jnp.stack(betas))
```

```python
import functools

import jax
import jax.numpy as jnp
from jax import lax
from jax.experimental import pallas as pl
from jax.experimental.pallas import tpu as pltpu
from jax.sharding import PartitionSpec as P

F32 = jnp.float32
BF16 = jnp.bfloat16
HIGH = lax.Precision.HIGHEST
TILE = 256
NN = (((1,), (0,)), ((), ()))
NT = (((1,), (1,)), ((), ()))


def fdot(a, b, dims=NN):
    return lax.dot_general(a, b, dims, precision=HIGH, preferred_element_type=F32)


def bdot(a, b, dims=NN):
    return lax.dot_general(a, b, dims, preferred_element_type=F32)


def halves(x):
    hi = x.astype(BF16)
    lo = (x - hi.astype(F32)).astype(BF16)
    return hi, lo


def lanes(blocks, width):
    used = sum(b.shape[1] for b in blocks)
    rows = blocks[0].shape[0]
    return jnp.concatenate([*blocks, jnp.zeros((rows, width - used), F32)], axis=1)


def block_of(stats, index):
    return stats[:, 16 * index : 16 * index + 16]


def wide(stats):
    return jnp.concatenate([stats[:8], stats[8:]], axis=1)


def tall(stats):
    return jnp.concatenate([stats[:, :128], stats[:, 128:]], axis=0)


def factor(gram):
    size = gram.shape[0]
    row = lax.broadcasted_iota(jnp.int32, (size, 1), 0)
    lane = lax.broadcasted_iota(jnp.int32, (size, size), 1)
    eye = jnp.where(lax.broadcasted_iota(jnp.int32, (size, size), 0) == lane, 1.0, 0.0)
    work, inv = gram, eye
    lower = jnp.zeros_like(gram)
    for k in range(size):
        pivot = work[k : k + 1, k : k + 1]
        r = lax.rsqrt(pivot)
        r = r * (1.5 - 0.5 * pivot * r * r)
        col = work[:, k : k + 1] * r
        lower = jnp.where((lane == k) & (row >= k), col, lower)
        below = jnp.where(row > k, col, 0.0)
        work_row = work[k : k + 1, :] * r
        inv_row = inv[k : k + 1, :] * r
        work = work - below * work_row
        inv = jnp.where(row == k, inv_row, inv - below * inv_row)
    return lower, inv


def orthonormal(onto, basis, own):
    count = len(onto)
    gram = own
    for l in range(count):
        part = -2.0 * onto[l]
        for m in range(count):
            if m >= l:
                part = part + fdot(onto[m], basis[m][l])
            else:
                part = part + fdot(onto[m], basis[l][m], NT)
        gram = gram + fdot(part, onto[l], NT)
    lower, inv = factor(gram)
    return lower, jnp.concatenate([inv] + [-fdot(inv, c) for c in onto], axis=1)


def added(ref):
    total = ref[0]
    for k in range(1, ref.shape[0]):
        total = total + ref[k]
    return total


def copies(ref, value):
    for k in range(ref.shape[0]):
        ref[k] = value


def gathered(ref):
    return jnp.concatenate([ref[k] for k in range(ref.shape[0])], axis=1)


def stack_of(*values):
    parts = [halves(v) for v in values]
    return jnp.concatenate([p[0] for p in parts] + [p[1] for p in parts], axis=0)


def products(x, y):
    m, k = x.shape[0] // 2, y.shape[0] // 2
    full = bdot(x, y, NT)
    return full[:m, :k] + (full[:m, k:] + full[m:, :k]) + full[m:, k:]


PARTS = 2


def first_pass(sp, sh, cp, cd, rho, lb, ln, *refs):
    matrix, (out, rows, st, ce, cxb, cyb, czb) = refs[: 2 * PARTS], refs[2 * PARTS :]
    n_s, n_c = st.shape[1], ce.shape[1]
    st[0:2, :] = sp[...].astype(F32)
    st[2:3, :] = sh[...].astype(F32) + 0.5
    ce[...] = jnp.zeros_like(ce)
    ce[0:2, :] = cp[...].astype(F32)
    ce[2:3, :] = cd[...].astype(F32)
    rows[...] = stack_of(ln[...], lb[...])
    gram = products(rows[...], rows[...])
    stats = lanes([gram[16:, 16:], gram[:16, 16:], gram[:16, :16]], 128)

    def both(ref, r0):
        return jnp.concatenate([ref[r0 : r0 + 8, :]] * 2, axis=1)

    def cell_block(part, cb, carry):
        hi_ref, lo_ref = matrix[2 * part], matrix[2 * part + 1]
        g0 = pl.multiple_of(cb * TILE, TILE)
        c0 = part * (n_c // PARTS) + g0
        for half in range(2):
            turned = jnp.transpose(ce[:, pl.ds(pl.multiple_of(c0 + 128 * half, 128), 128)])
            put = slice(128 * half, 128 * half + 128)
            cxb[put, :] = jnp.broadcast_to(turned[:, 0:1], (128, 128))
            cyb[put, :] = jnp.broadcast_to(turned[:, 1:2], (128, 128))
            czb[put, :] = jnp.broadcast_to(turned[:, 2:3], (128, 128))

        def station_block(sb, inner):
            here = pl.ds(pl.multiple_of(sb * TILE, TILE), TILE)
            sx = jnp.broadcast_to(st[0:1, here], (8, TILE))
            sy = jnp.broadcast_to(st[1:2, here], (8, TILE))
            sz = jnp.broadcast_to(st[2:3, here], (8, TILE))
            for r0 in range(0, TILE, 8):
                dx = sx - both(cxb, r0)
                dy = sy - both(cyb, r0)
                dz = sz + both(czb, r0)
                dz2 = dz * dz
                inv = lax.rsqrt(dx * dx + dy * dy + dz2)
                inv2 = inv * inv
                g = (dz2 * inv2 - (1.0 / 3.0)) * (inv2 * inv)
                g_hi = g.astype(BF16)
                where = pl.ds(pl.multiple_of(g0 + r0, 8), 8)
                hi_ref[where, here] = g_hi
                lo_ref[where, here] = (g - g_hi.astype(F32)).astype(BF16)
            return inner

        lax.fori_loop(0, n_s // TILE, station_block, 0)
        big = bdot(rows[...], hi_ref[pl.ds(g0, TILE), :], NT)
        small = bdot(rows[:32, :], lo_ref[pl.ds(g0, TILE), :], NT)
        total = (big[:32] + big[32:] + small) * (12.0 * rho[0:1, pl.ds(pl.multiple_of(c0, TILE), TILE)])
        for k in range(2):
            piece = 2 * cb + k + part * (n_c // PARTS // 128)
            out[piece, :32, :] = total[:, 128 * k : 128 * k + 128]
            out[piece, 32:, :] = stats
        return carry

    for part in range(PARTS):
        lax.fori_loop(0, n_c // PARTS // TILE, functools.partial(cell_block, part), 0)


def first_sum(rs, ag, keep):
    total = added(rs)
    keep[...] = total
    copies(ag, total[:16])


def forward_product(rows, count, matrix, out, stats):
    step = 2 * TILE
    size = matrix[0].shape[0]

    def station_block(sb, carry):
        s0 = pl.multiple_of(sb * step, step)
        total = jnp.zeros((count, step), F32)
        for part in range(PARTS):
            own = slice(part * size, part * size + size)
            big = bdot(rows[:, own], matrix[2 * part][:, pl.ds(s0, step)])
            small = bdot(rows[:count, own], matrix[2 * part + 1][:, pl.ds(s0, step)])
            total = total + (big[:count] + big[count:] + small)
        for k in range(2):
            out[2 * sb + k, :count, :] = total[:, TILE * k : TILE * k + TILE]
            out[2 * sb + k, count:, :] = stats
        return carry

    lax.fori_loop(0, matrix[0].shape[1] // step, station_block, 0)


def second_pass(ag, q, rho, *refs):
    matrix, (out, rows) = refs[: 2 * PARTS], refs[2 * PARTS :]
    w = gathered(ag)
    base = q[...]
    scale = 12.0 * rho[...]
    rows[...] = stack_of(w * scale, base * scale)
    pair = stack_of(w, base)
    gram = products(pair, pair)
    stats = lanes([gram[16:, 16:], gram[:16, 16:], gram[:16, :16]], 128)
    forward_product(rows, 32, matrix, out, wide(stats))


def second_sum(cells, rs, ag, keep, stats_out, t_out, l_out):
    total = added(rs)
    stats = tall(total[32:]) * (1.0 / cells)
    stats_out[...] = stats
    lower, t = orthonormal([block_of(stats, 1)], [[block_of(stats, 0)]], block_of(stats, 2))
    l_out[...] = lower
    t_out[...] = t
    v = fdot(t, total[:32])
    keep[...] = jnp.concatenate([v, total[16:32]], axis=0)
    copies(ag, v)


def third_pass(ag, left_rows, rho, *refs):
    matrix, (out, rows) = refs[: 2 * PARTS], refs[2 * PARTS :]
    v = gathered(ag)
    rows[...] = stack_of(v)
    gram = products(rows[...], left_rows[...])
    stats = lanes([gram[:, 16:], gram[:, :16], products(rows[...], rows[...])], 128)

    size = matrix[0].shape[0]

    def cell_block(part, cb, carry):
        g0 = pl.multiple_of(cb * TILE, TILE)
        c0 = pl.multiple_of(part * size + g0, TILE)
        big = bdot(rows[...], matrix[2 * part][pl.ds(g0, TILE), :], NT)
        small = bdot(rows[:16, :], matrix[2 * part + 1][pl.ds(g0, TILE), :], NT)
        total = (big[:16] + big[16:] + small) * (12.0 * rho[0:1, pl.ds(c0, TILE)])
        for k in range(2):
            piece = 2 * cb + k + part * (size // 128)
            out[piece, :16, :] = total[:, 128 * k : 128 * k + 128]
            out[piece, 16:, :] = stats
        return carry

    for part in range(PARTS):
        lax.fori_loop(0, size // TILE, functools.partial(cell_block, part), 0)


def third_sum(stations, rs, keep0, ag, t_out, l_out):
    total = added(rs)
    stats = total[16:] * (1.0 / stations)
    base = keep0[32:48, :] * (1.0 / stations)
    grams = [[block_of(base, 0)], [block_of(base, 1), block_of(base, 2)]]
    lower, t = orthonormal([block_of(stats, 0), block_of(stats, 1)], grams, block_of(stats, 2))
    l_out[...] = lower
    t_out[...] = t
    w = fdot(t, jnp.concatenate([total[:16], keep0[16:32, :], keep0[:16, :]], axis=0))
    copies(ag, w)


def fourth_pass(ag2, ag0, q, rho, t1, *refs):
    matrix, (right_out, out, rows) = refs[: 2 * PARTS], refs[2 * PARTS :]
    base = q[...]
    right = fdot(t1[...], jnp.concatenate([gathered(ag0), base], axis=0))
    right_out[...] = right
    w = gathered(ag2)
    rows[...] = stack_of(w * (12.0 * rho[...]))
    gram = products(stack_of(right, w), stack_of(base, right, w))
    stats = lanes([gram[:16, :32], gram[16:, :48]], 128)
    forward_product(rows, 16, matrix, out, wide(stats))


def fourth_sum(cells, rs, keep1, stats1, ag, t_out, l_out):
    total = added(rs)
    stats = tall(total[16:]) * (1.0 / cells)
    grams = [[block_of(stats1[...], 0)], [block_of(stats, 0), block_of(stats, 1)]]
    lower, t = orthonormal([block_of(stats, 2), block_of(stats, 3)], grams, block_of(stats, 4))
    l_out[...] = lower
    t_out[...] = t
    v = fdot(t, jnp.concatenate([total[:16], keep1[16:, :], keep1[:16, :]], axis=0))
    copies(ag, v)


def last_stats(ag3, ag1, lb, ln, t2, left_out, out):
    before, now = lb[...], ln[...]
    left = fdot(t2[...], jnp.concatenate([gathered(ag1), before, now], axis=0))
    left_out[...] = left
    v = gathered(ag3)
    gram = products(stack_of(left, v), stack_of(before, now, left, v))
    copies(out, lanes([gram[:16, :48], gram[16:, :64]], 128))


def finish(stations, rs, keep0, ag3, lb, ln, left1, ag2, q, right1, t3, l1, l2, l3, rights, left_out, alphas, betas):
    stats = added(rs) * (1.0 / stations)
    base = keep0[32:48, :] * (1.0 / stations)
    grams = [
        [block_of(base, 0)],
        [block_of(base, 1), block_of(base, 2)],
        [block_of(stats, 0), block_of(stats, 1), block_of(stats, 2)],
    ]
    onto = [block_of(stats, 3), block_of(stats, 4), block_of(stats, 5)]
    lower, t = orthonormal(onto, grams, block_of(stats, 6))
    left_out[...] = fdot(t, jnp.concatenate([gathered(ag3), lb[...], ln[...], left1[...]], axis=0))
    rights[0] = right1[...]
    rights[1] = fdot(t3[...], jnp.concatenate([gathered(ag2), q[...], right1[...]], axis=0))
    alphas[0] = l1[...]
    alphas[1] = l3[...]
    betas[0] = l2[...]
    betas[1] = lower


def call(kernel, args, outs, scratch=(), limit=4):
    spec = pl.BlockSpec(memory_space=pltpu.VMEM)
    return pl.pallas_call(
        kernel,
        out_shape=tuple(outs),
        in_specs=[spec] * len(args),
        out_specs=tuple(spec for _ in outs),
        scratch_shapes=list(scratch),
        compiler_params=pltpu.CompilerParams(vmem_limit_bytes=limit * 2**20),
    )(*args)


def f32(*shape):
    return jax.ShapeDtypeStruct(shape, F32)


def exchange(value, axis):
    return lax.all_to_all(value, axis, split_axis=0, concat_axis=0, tiled=True)


def body(station_plane, station_height, cell_plane, cell_depth, cell_density, left_before, left_now, right_before):
    n_s, n_c = left_now.shape[1], right_before.shape[1]
    n_sta, n_cel = lax.axis_size("sta"), lax.axis_size("cel")
    stations, cells = n_s * n_sta, n_c * n_cel
    cp, sp = n_c // n_sta, n_s // n_cel
    lb, ln, q = left_before, left_now, right_before
    rho = cell_density.reshape(1, n_c)
    small = f32(16, 16)

    *matrix, rs0, left_rows = call(
        first_pass,
        (
            station_plane,
            station_height.reshape(1, n_s),
            cell_plane,
            cell_depth.reshape(1, n_c),
            rho,
            lb,
            ln,
        ),
        (
            *[pltpu.VMEM((n_c // PARTS, n_s), BF16)] * (2 * PARTS),
            f32(n_sta, 48, cp),
            pltpu.VMEM((64, n_s), BF16),
        ),
        [
            pltpu.VMEM((8, n_s), F32),
            pltpu.VMEM((8, n_c), F32),
            pltpu.VMEM((TILE, 128), F32),
            pltpu.VMEM((TILE, 128), F32),
            pltpu.VMEM((TILE, 128), F32),
        ],
    )
    ag0, keep0 = call(first_sum, (exchange(rs0, "sta"),), (f32(n_sta, 16, cp), f32(48, cp)))
    ag0 = exchange(ag0, "sta")
    (rs1,) = call(second_pass, (ag0, q, rho, *matrix), (f32(n_cel, 40, sp),), [pltpu.VMEM((64, n_c), BF16)])
    ag1, keep1, stats1, t1, l1 = call(
        lambda *refs: second_sum(cells, *refs),
        (exchange(rs1, "cel"),),
        (f32(n_cel, 16, sp), f32(32, sp), f32(16, 128), f32(16, 32), small),
    )
    ag1 = exchange(ag1, "cel")
    (rs2,) = call(third_pass, (ag1, left_rows, rho, *matrix), (f32(n_sta, 32, cp),), [pltpu.VMEM((32, n_s), BF16)])
    ag2, t2, l2 = call(
        lambda *refs: third_sum(stations, *refs),
        (exchange(rs2, "sta"), keep0),
        (f32(n_sta, 16, cp), f32(16, 48), small),
    )
    ag2 = exchange(ag2, "sta")
    right1, rs3 = call(
        fourth_pass,
        (ag2, ag0, q, rho, t1, *matrix),
        (f32(16, n_c), f32(n_cel, 24, sp)),
        [pltpu.VMEM((32, n_c), BF16)],
    )
    ag3, t3, l3 = call(
        lambda *refs: fourth_sum(cells, *refs),
        (exchange(rs3, "cel"), keep1, stats1),
        (f32(n_cel, 16, sp), f32(16, 48), small),
    )
    ag3 = exchange(ag3, "cel")
    left1, rs4 = call(last_stats, (ag3, ag1, lb, ln, t2), (f32(16, n_s), f32(n_sta, 16, 128)))
    rights, left2, alphas, betas = call(
        lambda *refs: finish(stations, *refs),
        (exchange(rs4, "sta"), keep0, ag3, lb, ln, left1, ag2, q, right1, t3, l1, l2, l3),
        (f32(2, 16, n_c), f32(16, n_s), f32(2, 16, 16), f32(2, 16, 16)),
    )
    return rights, left2, alphas, betas


def solution(mesh):
    in_specs = (
        P(None, "sta"),
        P("sta"),
        P(None, "cel"),
        P("cel"),
        P("cel"),
        P(None, "sta"),
        P(None, "sta"),
        P(None, "cel"),
    )
    out_specs = (P(None, None, "cel"), P(None, "sta"), P(), P())
    return jax.shard_map(body, mesh=mesh, in_specs=in_specs, out_specs=out_specs, check_vma=False)
```

```python
import functools

import jax
import jax.numpy as jnp
from jax import lax
from jax.experimental import pallas as pl
from jax.experimental.pallas import tpu as pltpu
from jax.sharding import PartitionSpec as P

F32 = jnp.float32
BF16 = jnp.bfloat16
HIGH = lax.Precision.HIGHEST
TILE = 256
NN = (((1,), (0,)), ((), ()))
NT = (((1,), (1,)), ((), ()))


def fdot(a, b, dims=NN):
    return lax.dot_general(a, b, dims, precision=HIGH, preferred_element_type=F32)


def bdot(a, b, dims=NN):
    return lax.dot_general(a, b, dims, preferred_element_type=F32)


def halves(x):
    hi = x.astype(BF16)
    lo = (x - hi.astype(F32)).astype(BF16)
    return hi, lo


def lanes(blocks, width):
    used = sum(b.shape[1] for b in blocks)
    rows = blocks[0].shape[0]
    return jnp.concatenate([*blocks, jnp.zeros((rows, width - used), F32)], axis=1)


def block_of(stats, index):
    return stats[:, 16 * index : 16 * index + 16]


def wide(stats):
    return jnp.concatenate([stats[:8], stats[8:]], axis=1)


def tall(stats):
    return jnp.concatenate([stats[:, :128], stats[:, 128:]], axis=0)


def factor(gram):
    size = gram.shape[0]
    row = lax.broadcasted_iota(jnp.int32, (size, 1), 0)
    lane = lax.broadcasted_iota(jnp.int32, (size, size), 1)
    eye = jnp.where(lax.broadcasted_iota(jnp.int32, (size, size), 0) == lane, 1.0, 0.0)
    work, inv = gram, eye
    lower = jnp.zeros_like(gram)
    for k in range(size):
        pivot = work[k : k + 1, k : k + 1]
        r = lax.rsqrt(pivot)
        r = r * (1.5 - 0.5 * pivot * r * r)
        col = work[:, k : k + 1] * r
        lower = jnp.where((lane == k) & (row >= k), col, lower)
        below = jnp.where(row > k, col, 0.0)
        work_row = work[k : k + 1, :] * r
        inv_row = inv[k : k + 1, :] * r
        work = work - below * work_row
        inv = jnp.where(row == k, inv_row, inv - below * inv_row)
    return lower, inv


def orthonormal(onto, basis, own):
    count = len(onto)
    gram = own
    for l in range(count):
        part = -2.0 * onto[l]
        for m in range(count):
            if m >= l:
                part = part + fdot(onto[m], basis[m][l])
            else:
                part = part + fdot(onto[m], basis[l][m], NT)
        gram = gram + fdot(part, onto[l], NT)
    lower, inv = factor(gram)
    return lower, jnp.concatenate([inv] + [-fdot(inv, c) for c in onto], axis=1)


def added(ref):
    total = ref[0]
    for k in range(1, ref.shape[0]):
        total = total + ref[k]
    return total


def copies(ref, value):
    for k in range(ref.shape[0]):
        ref[k] = value


def gathered(ref):
    return jnp.concatenate([ref[k] for k in range(ref.shape[0])], axis=1)


def stack_of(*values):
    parts = [halves(v) for v in values]
    return jnp.concatenate([p[0] for p in parts] + [p[1] for p in parts], axis=0)


def products(x, y):
    m, k = x.shape[0] // 2, y.shape[0] // 2
    full = bdot(x, y, NT)
    return full[:m, :k] + (full[:m, k:] + full[m:, :k]) + full[m:, k:]


PARTS = 2
LARGE = 62


def pieces(x):
    first = x.astype(BF16).astype(F32)
    second = (x - first).astype(BF16).astype(F32)
    return [first, second, x - first - second]


def fetch(*refs):
    count = len(refs) // 2
    sems = refs[-1]
    moves = [pltpu.make_async_copy(refs[k], refs[count + k], sems.at[k]) for k in range(count)]
    for move in moves:
        move.start()
    for move in moves:
        move.wait()


def first_pass(sp_v, sh_v, cp_v, cd_v, rho_v, lb_v, ln_v, *refs):
    matrix, refs = refs[: 2 * PARTS], refs[2 * PARTS :]
    out, rows, sz_v, czb, a_ref, b_ref, square = refs
    n_s, n_c = sp_v.shape[1], cp_v.shape[1]

    sx, sy = sp_v[0:1, :].astype(F32), sp_v[1:2, :].astype(F32)
    sz = sh_v[...].astype(F32) + 0.5
    sz_v[...] = jnp.broadcast_to(sz, sz_v.shape)
    one, zero = jnp.ones_like(sx), jnp.zeros_like(sx)
    b_rows = pieces(sx * sx + sy * sy + sz * sz) + [one, one, one, -2.0 * sx, -2.0 * sy, 2.0 * sz] + [zero] * 7
    b_ref[...] = jnp.concatenate(b_rows, axis=0).astype(BF16)

    rows[...] = stack_of(ln_v[...], lb_v[...])
    gram = products(rows[...], rows[...])
    stats = lanes([gram[16:, 16:], gram[:16, 16:], gram[:16, :16]], 128)

    def prepare(c0):
        for half in range(2):
            here = pl.ds(pl.multiple_of(c0 + 128 * half, 128), 128)
            put = slice(128 * half, 128 * half + 128)
            cx, cy = cp_v[0:1, here].astype(F32), cp_v[1:2, here].astype(F32)
            cz = cd_v[0:1, here].astype(F32)
            unit, none = jnp.ones_like(cx), jnp.zeros_like(cx)
            a_rows = [unit, unit, unit] + pieces(cx * cx + cy * cy + cz * cz) + [cx, cy, cz] + [none] * 7
            turned = jnp.transpose(jnp.concatenate(a_rows, axis=0))
            a_ref[put, :] = turned.astype(BF16)
            czb[put, :] = jnp.broadcast_to(turned[:, 8:9], (128, 128))

    def cell_block(part, cb, carry):
        hi_ref, lo_ref = matrix[2 * part], matrix[2 * part + 1]
        g0 = pl.multiple_of(cb * TILE, TILE)
        c0 = pl.multiple_of(part * (n_c // PARTS) + g0, TILE)

        def station_block(sb, inner):
            for half in range(2):
                here = pl.ds(pl.multiple_of(sb * 2 * TILE + half * TILE, TILE), TILE)
                height = sz_v[:, here]
                for r0 in range(0, TILE, 8):
                    dz = height + jnp.concatenate([czb[r0 : r0 + 8, :]] * 2, axis=1)
                    inv = lax.rsqrt(square[r0 : r0 + 8, here])
                    inv2 = inv * inv
                    g = (dz * dz * inv2 - (1.0 / 3.0)) * (inv2 * inv)
                    where = pl.ds(pl.multiple_of(g0 + r0, 8), 8)
                    hi_ref[where, here] = g.astype(BF16)
                    lo_ref[where, here] = (g - hi_ref[where, here].astype(F32)).astype(BF16)
            return inner

        lax.fori_loop(0, n_s // (2 * TILE), station_block, 0)
        prepare(jnp.minimum(c0 + TILE, n_c - TILE))
        big = bdot(rows[...], hi_ref[pl.ds(g0, TILE), :], NT)
        small = bdot(rows[:32, :], lo_ref[pl.ds(g0, TILE), :], NT)
        total = (big[:32] + big[32:] + small) * (12.0 * rho_v[0:1, pl.ds(c0, TILE)])
        for k in range(2):
            piece = 2 * cb + k + part * (n_c // PARTS // 128)
            out[piece, :32, :] = total[:, 128 * k : 128 * k + 128]
            out[piece, 32:, :] = stats
        square[...] = bdot(a_ref[...], b_ref[...])
        return carry

    prepare(0)
    square[...] = bdot(a_ref[...], b_ref[...])
    for part in range(PARTS):
        lax.fori_loop(0, n_c // PARTS // TILE, functools.partial(cell_block, part), 0)


def first_sum(rs, ag, keep):
    total = added(rs)
    keep[...] = total
    copies(ag, total[:16])


def forward_product(rows, count, matrix, out, stats):
    step = 2 * TILE
    size = matrix[0].shape[0]

    def station_block(sb, carry):
        s0 = pl.multiple_of(sb * step, step)
        total = jnp.zeros((count, step), F32)
        for part in range(PARTS):
            own = slice(part * size, part * size + size)
            big = bdot(rows[:, own], matrix[2 * part][:, pl.ds(s0, step)])
            small = bdot(rows[:count, own], matrix[2 * part + 1][:, pl.ds(s0, step)])
            total = total + (big[:count] + big[count:] + small)
        for k in range(2):
            out[2 * sb + k, :count, :] = total[:, TILE * k : TILE * k + TILE]
            out[2 * sb + k, count:, :] = stats
        return carry

    lax.fori_loop(0, matrix[0].shape[1] // step, station_block, 0)


def second_pass(ag, q, rho, *refs):
    matrix, (out, rows) = refs[: 2 * PARTS], refs[2 * PARTS :]
    w = gathered(ag)
    base = q[...]
    scale = 12.0 * rho[...]
    rows[...] = stack_of(w * scale, base * scale)
    pair = stack_of(w, base)
    gram = products(pair, pair)
    stats = lanes([gram[16:, 16:], gram[:16, 16:], gram[:16, :16]], 128)
    forward_product(rows, 32, matrix, out, wide(stats))


def second_sum(cells, rs, ag, keep, stats_out, t_out, l_out):
    total = added(rs)
    stats = tall(total[32:]) * (1.0 / cells)
    stats_out[...] = stats
    lower, t = orthonormal([block_of(stats, 1)], [[block_of(stats, 0)]], block_of(stats, 2))
    l_out[...] = lower
    t_out[...] = t
    v = fdot(t, total[:32])
    keep[...] = jnp.concatenate([v, total[16:32]], axis=0)
    copies(ag, v)


def third_pass(ag, left_rows, rho, *refs):
    matrix, (out, rows) = refs[: 2 * PARTS], refs[2 * PARTS :]
    v = gathered(ag)
    rows[...] = stack_of(v)
    gram = products(rows[...], left_rows[...])
    stats = lanes([gram[:, 16:], gram[:, :16], products(rows[...], rows[...])], 128)

    size = matrix[0].shape[0]

    def cell_block(part, cb, carry):
        g0 = pl.multiple_of(cb * TILE, TILE)
        c0 = pl.multiple_of(part * size + g0, TILE)
        big = bdot(rows[...], matrix[2 * part][pl.ds(g0, TILE), :], NT)
        small = bdot(rows[:16, :], matrix[2 * part + 1][pl.ds(g0, TILE), :], NT)
        total = (big[:16] + big[16:] + small) * (12.0 * rho[0:1, pl.ds(c0, TILE)])
        for k in range(2):
            piece = 2 * cb + k + part * (size // 128)
            out[piece, :16, :] = total[:, 128 * k : 128 * k + 128]
            out[piece, 16:, :] = stats
        return carry

    for part in range(PARTS):
        lax.fori_loop(0, size // TILE, functools.partial(cell_block, part), 0)


def third_sum(stations, rs, keep0, ag, t_out, l_out):
    total = added(rs)
    stats = total[16:] * (1.0 / stations)
    base = keep0[32:48, :] * (1.0 / stations)
    grams = [[block_of(base, 0)], [block_of(base, 1), block_of(base, 2)]]
    lower, t = orthonormal([block_of(stats, 0), block_of(stats, 1)], grams, block_of(stats, 2))
    l_out[...] = lower
    t_out[...] = t
    w = fdot(t, jnp.concatenate([total[:16], keep0[16:32, :], keep0[:16, :]], axis=0))
    copies(ag, w)


def fourth_pass(ag2, ag0, q, rho, t1, *refs):
    matrix, (right_out, out, rows) = refs[: 2 * PARTS], refs[2 * PARTS :]
    base = q[...]
    right = fdot(t1[...], jnp.concatenate([gathered(ag0), base], axis=0))
    right_out[...] = right
    w = gathered(ag2)
    rows[...] = stack_of(w * (12.0 * rho[...]))
    gram = products(stack_of(right, w), stack_of(base, right, w))
    stats = lanes([gram[:16, :32], gram[16:, :48]], 128)
    forward_product(rows, 16, matrix, out, wide(stats))


def fourth_sum(cells, rs, keep1, stats1, ag, t_out, l_out):
    total = added(rs)
    stats = tall(total[16:]) * (1.0 / cells)
    grams = [[block_of(stats1[...], 0)], [block_of(stats, 0), block_of(stats, 1)]]
    lower, t = orthonormal([block_of(stats, 2), block_of(stats, 3)], grams, block_of(stats, 4))
    l_out[...] = lower
    t_out[...] = t
    v = fdot(t, jnp.concatenate([total[:16], keep1[16:, :], keep1[:16, :]], axis=0))
    copies(ag, v)


def last_stats(ag3, ag1, lb, ln, t2, left_out, out):
    before, now = lb[...], ln[...]
    left = fdot(t2[...], jnp.concatenate([gathered(ag1), before, now], axis=0))
    left_out[...] = left
    v = gathered(ag3)
    gram = products(stack_of(left, v), stack_of(before, now, left, v))
    copies(out, lanes([gram[:16, :48], gram[16:, :64]], 128))


def finish(stations, rs, keep0, ag3, lb, ln, left1, ag2, q, right1, t3, l1, l2, l3, rights, left_out, alphas, betas):
    stats = added(rs) * (1.0 / stations)
    base = keep0[32:48, :] * (1.0 / stations)
    grams = [
        [block_of(base, 0)],
        [block_of(base, 1), block_of(base, 2)],
        [block_of(stats, 0), block_of(stats, 1), block_of(stats, 2)],
    ]
    onto = [block_of(stats, 3), block_of(stats, 4), block_of(stats, 5)]
    lower, t = orthonormal(onto, grams, block_of(stats, 6))
    left_out[...] = fdot(t, jnp.concatenate([gathered(ag3), lb[...], ln[...], left1[...]], axis=0))
    rights[0] = right1[...]
    rights[1] = fdot(t3[...], jnp.concatenate([gathered(ag2), q[...], right1[...]], axis=0))
    alphas[0] = l1[...]
    alphas[1] = l3[...]
    betas[0] = l2[...]
    betas[1] = lower


def call(kernel, args, outs, scratch=(), limit=4, where=pltpu.VMEM):
    spec = pl.BlockSpec(memory_space=pltpu.VMEM)
    return pl.pallas_call(
        kernel,
        out_shape=tuple(outs),
        in_specs=[pl.BlockSpec(memory_space=where)] * len(args),
        out_specs=tuple(spec for _ in outs),
        scratch_shapes=list(scratch),
        compiler_params=pltpu.CompilerParams(vmem_limit_bytes=limit * 2**20),
    )(*args)


def f32(*shape):
    return jax.ShapeDtypeStruct(shape, F32)


def exchange(value, axis):
    return lax.all_to_all(value, axis, split_axis=0, concat_axis=0, tiled=True)


def body(station_plane, station_height, cell_plane, cell_depth, cell_density, left_before, left_now, right_before):
    n_s, n_c = left_now.shape[1], right_before.shape[1]
    n_sta, n_cel = lax.axis_size("sta"), lax.axis_size("cel")
    stations, cells = n_s * n_sta, n_c * n_cel
    cp, sp = n_c // n_sta, n_s // n_cel
    small = f32(16, 16)

    inputs = (
        station_plane,
        station_height.reshape(1, n_s),
        cell_plane,
        cell_depth.reshape(1, n_c),
        cell_density.reshape(1, n_c),
        left_before,
        left_now,
        right_before,
    )
    sp_v, sh_v, cp_v, cd_v, rho, lb, ln, q = call(
        fetch,
        inputs,
        [pltpu.VMEM(v.shape, v.dtype) for v in inputs],
        [pltpu.SemaphoreType.DMA((len(inputs),))],
        limit=LARGE,
        where=pltpu.HBM,
    )
    *matrix, rs0, left_rows = call(
        first_pass,
        (sp_v, sh_v, cp_v, cd_v, rho, lb, ln),
        (
            *[pltpu.VMEM((n_c // PARTS, n_s), BF16)] * (2 * PARTS),
            f32(n_sta, 48, cp),
            pltpu.VMEM((64, n_s), BF16),
        ),
        [
            pltpu.VMEM((8, n_s), F32),
            pltpu.VMEM((TILE, 128), F32),
            pltpu.VMEM((TILE, 16), BF16),
            pltpu.VMEM((16, n_s), BF16),
            pltpu.VMEM((TILE, n_s), F32),
        ],
        limit=10,
    )
    ag0, keep0 = call(first_sum, (exchange(rs0, "sta"),), (f32(n_sta, 16, cp), f32(48, cp)))
    ag0 = exchange(ag0, "sta")
    (rs1,) = call(second_pass, (ag0, q, rho, *matrix), (f32(n_cel, 40, sp),), [pltpu.VMEM((64, n_c), BF16)])
    ag1, keep1, stats1, t1, l1 = call(
        lambda *refs: second_sum(cells, *refs),
        (exchange(rs1, "cel"),),
        (f32(n_cel, 16, sp), f32(32, sp), f32(16, 128), f32(16, 32), small),
    )
    ag1 = exchange(ag1, "cel")
    (rs2,) = call(third_pass, (ag1, left_rows, rho, *matrix), (f32(n_sta, 32, cp),), [pltpu.VMEM((32, n_s), BF16)])
    ag2, t2, l2 = call(
        lambda *refs: third_sum(stations, *refs),
        (exchange(rs2, "sta"), keep0),
        (f32(n_sta, 16, cp), f32(16, 48), small),
    )
    ag2 = exchange(ag2, "sta")
    right1, rs3 = call(
        fourth_pass,
        (ag2, ag0, q, rho, t1, *matrix),
        (f32(16, n_c), f32(n_cel, 24, sp)),
        [pltpu.VMEM((32, n_c), BF16)],
    )
    ag3, t3, l3 = call(
        lambda *refs: fourth_sum(cells, *refs),
        (exchange(rs3, "cel"), keep1, stats1),
        (f32(n_cel, 16, sp), f32(16, 48), small),
    )
    ag3 = exchange(ag3, "cel")
    left1, rs4 = call(last_stats, (ag3, ag1, lb, ln, t2), (f32(16, n_s), f32(n_sta, 16, 128)))
    rights, left2, alphas, betas = call(
        lambda *refs: finish(stations, *refs),
        (exchange(rs4, "sta"), keep0, ag3, lb, ln, left1, ag2, q, right1, t3, l1, l2, l3),
        (f32(2, 16, n_c), f32(16, n_s), f32(2, 16, 16), f32(2, 16, 16)),
    )
    return rights, left2, alphas, betas


def solution(mesh):
    in_specs = (
        P(None, "sta"),
        P("sta"),
        P(None, "cel"),
        P("cel"),
        P("cel"),
        P(None, "sta"),
        P(None, "sta"),
        P(None, "cel"),
    )
    out_specs = (P(None, None, "cel"), P(None, "sta"), P(), P())
    return jax.shard_map(body, mesh=mesh, in_specs=in_specs, out_specs=out_specs, check_vma=False)
```

```python
import functools

import jax
import jax.numpy as jnp
from jax import lax
from jax.experimental import pallas as pl
from jax.experimental.pallas import tpu as pltpu
from jax.sharding import PartitionSpec as P

F32 = jnp.float32
BF16 = jnp.bfloat16
HIGH = lax.Precision.HIGHEST
TILE = 256
NN = (((1,), (0,)), ((), ()))
NT = (((1,), (1,)), ((), ()))


def fdot(a, b, dims=NN):
    return lax.dot_general(a, b, dims, precision=HIGH, preferred_element_type=F32)


def bdot(a, b, dims=NN):
    return lax.dot_general(a, b, dims, preferred_element_type=F32)


def halves(x):
    hi = x.astype(BF16)
    lo = (x - hi.astype(F32)).astype(BF16)
    return hi, lo


def lanes(blocks, width):
    used = sum(b.shape[1] for b in blocks)
    rows = blocks[0].shape[0]
    return jnp.concatenate([*blocks, jnp.zeros((rows, width - used), F32)], axis=1)


def block_of(stats, index):
    return stats[:, 16 * index : 16 * index + 16]


def wide(stats):
    return lanes([stats[:8], stats[8:]], 128)


def tall(tile):
    return jnp.concatenate([tile[:, :48], tile[:, 48:96]], axis=0)


def unfolded(message, count):
    return jnp.concatenate([message[:, 256 * k : 256 * k + 256] for k in range(count // 8)], axis=0)


def factor(gram):
    size = gram.shape[0]
    row = lax.broadcasted_iota(jnp.int32, (size, 1), 0)
    lane = lax.broadcasted_iota(jnp.int32, (size, size), 1)
    eye = jnp.where(lax.broadcasted_iota(jnp.int32, (size, size), 0) == lane, 1.0, 0.0)
    work, inv = gram, eye
    lower = jnp.zeros_like(gram)
    for k in range(size):
        pivot = work[k : k + 1, k : k + 1]
        r = lax.rsqrt(pivot)
        r = r * (1.5 - 0.5 * pivot * r * r)
        col = work[:, k : k + 1] * r
        lower = jnp.where((lane == k) & (row >= k), col, lower)
        below = jnp.where(row > k, col, 0.0)
        work_row = work[k : k + 1, :] * r
        inv_row = inv[k : k + 1, :] * r
        work = work - below * work_row
        inv = jnp.where(row == k, inv_row, inv - below * inv_row)
    return lower, inv


def orthonormal(onto, basis, own):
    count = len(onto)
    gram = own
    for l in range(count):
        part = -2.0 * onto[l]
        for m in range(count):
            if m >= l:
                part = part + fdot(onto[m], basis[m][l])
            else:
                part = part + fdot(onto[m], basis[l][m], NT)
        gram = gram + fdot(part, onto[l], NT)
    lower, inv = factor(gram)
    return lower, jnp.concatenate([inv] + [-fdot(inv, c) for c in onto], axis=1)


def added(ref):
    total = ref[0]
    for k in range(1, ref.shape[0]):
        total = total + ref[k]
    return total


def copies(ref, value):
    for k in range(ref.shape[0]):
        ref[k] = value


def gathered(ref):
    return jnp.concatenate([ref[k] for k in range(ref.shape[0])], axis=1)


def stack_of(*values):
    parts = [halves(v) for v in values]
    return jnp.concatenate([p[0] for p in parts] + [p[1] for p in parts], axis=0)


def products(x, y):
    m, k = x.shape[0] // 2, y.shape[0] // 2
    full = bdot(x, y, NT)
    return full[:m, :k] + (full[:m, k:] + full[m:, :k]) + full[m:, k:]


PARTS = 2
LARGE = 62


def pieces(x):
    first = x.astype(BF16).astype(F32)
    second = (x - first).astype(BF16).astype(F32)
    return [first, second, x - first - second]


def fetch(*refs):
    count = len(refs) // 2
    sems = refs[-1]
    moves = [pltpu.make_async_copy(refs[k], refs[count + k], sems.at[k]) for k in range(count)]
    for move in moves:
        move.start()
    for move in moves:
        move.wait()


def first_pass(sp_v, sh_v, cp_v, cd_v, rho_v, lb_v, ln_v, *refs):
    matrix, refs = refs[: 2 * PARTS], refs[2 * PARTS :]
    out, rows, stats_out, sz_v, czb, a_ref, b_ref, square = refs
    n_s, n_c = sp_v.shape[1], cp_v.shape[1]

    sx, sy = sp_v[0:1, :].astype(F32), sp_v[1:2, :].astype(F32)
    sz = sh_v[...].astype(F32) + 0.5
    sz_v[...] = jnp.broadcast_to(sz, sz_v.shape)
    one, zero = jnp.ones_like(sx), jnp.zeros_like(sx)
    b_rows = pieces(sx * sx + sy * sy + sz * sz) + [one, one, one, -2.0 * sx, -2.0 * sy, 2.0 * sz] + [zero] * 7
    b_ref[...] = jnp.concatenate(b_rows, axis=0).astype(BF16)

    rows[...] = stack_of(ln_v[...], lb_v[...])
    gram = products(rows[...], rows[...])
    stats_out[...] = lanes([gram[16:, 16:], gram[:16, 16:], gram[:16, :16]], 128)

    def prepare(c0):
        for half in range(2):
            here = pl.ds(pl.multiple_of(c0 + 128 * half, 128), 128)
            put = slice(128 * half, 128 * half + 128)
            cx, cy = cp_v[0:1, here].astype(F32), cp_v[1:2, here].astype(F32)
            cz = cd_v[0:1, here].astype(F32)
            unit, none = jnp.ones_like(cx), jnp.zeros_like(cx)
            a_rows = [unit, unit, unit] + pieces(cx * cx + cy * cy + cz * cz) + [cx, cy, cz] + [none] * 7
            turned = jnp.transpose(jnp.concatenate(a_rows, axis=0))
            a_ref[put, :] = turned.astype(BF16)
            czb[put, :] = jnp.broadcast_to(turned[:, 8:9], (128, 128))

    def cell_block(part, cb, carry):
        hi_ref, lo_ref = matrix[2 * part], matrix[2 * part + 1]
        g0 = pl.multiple_of(cb * TILE, TILE)
        c0 = pl.multiple_of(part * (n_c // PARTS) + g0, TILE)

        def station_block(sb, inner):
            for half in range(2):
                here = pl.ds(pl.multiple_of(sb * 2 * TILE + half * TILE, TILE), TILE)
                height = sz_v[:, here]
                for r0 in range(0, TILE, 8):
                    dz = height + jnp.concatenate([czb[r0 : r0 + 8, :]] * 2, axis=1)
                    inv = lax.rsqrt(square[r0 : r0 + 8, here])
                    inv2 = inv * inv
                    g = (dz * dz * inv2 - (1.0 / 3.0)) * (inv2 * inv)
                    where = pl.ds(pl.multiple_of(g0 + r0, 8), 8)
                    hi_ref[where, here] = g.astype(BF16)
                    lo_ref[where, here] = (g - hi_ref[where, here].astype(F32)).astype(BF16)
            return inner

        lax.fori_loop(0, n_s // (2 * TILE), station_block, 0)
        prepare(jnp.minimum(c0 + TILE, n_c - TILE))
        big = bdot(rows[...], hi_ref[pl.ds(g0, TILE), :], NT)
        small = bdot(rows[:32, :], lo_ref[pl.ds(g0, TILE), :], NT)
        total = (big[:32] + big[32:] + small) * (12.0 * rho_v[0:1, pl.ds(c0, TILE)])
        for k in range(2):
            piece = 2 * cb + k + part * (n_c // PARTS // 128)
            out[piece] = total[:, 128 * k : 128 * k + 128]
        square[...] = bdot(a_ref[...], b_ref[...])
        return carry

    prepare(0)
    square[...] = bdot(a_ref[...], b_ref[...])
    for part in range(PARTS):
        lax.fori_loop(0, n_c // PARTS // TILE, functools.partial(cell_block, part), 0)


def first_sum(rs, ag, keep):
    total = added(rs)
    keep[...] = total
    copies(ag, total[:16])


def forward_product(rows, count, matrix, out, stats):
    step = 4 * TILE
    size = matrix[0].shape[0]
    tile = wide(stats)

    def station_block(sb, carry):
        s0 = pl.multiple_of(sb * step, step)
        total = jnp.zeros((count, step), F32)
        for part in range(PARTS):
            own = slice(part * size, part * size + size)
            big = bdot(rows[:, own], matrix[2 * part][:, pl.ds(s0, step)])
            small = bdot(rows[:count, own], matrix[2 * part + 1][:, pl.ds(s0, step)])
            total = total + (big[:count] + big[count:] + small)
        for k in range(step // TILE):
            piece = sb * (step // TILE) + k
            for r in range(count // 8):
                out[piece, :, 256 * r : 256 * r + 256] = total[8 * r : 8 * r + 8, TILE * k : TILE * k + TILE]
            out[piece, :, 32 * count :] = tile
        return carry

    lax.fori_loop(0, matrix[0].shape[1] // step, station_block, 0)


def second_pass(ag, q, rho, *refs):
    matrix, (out, rows) = refs[: 2 * PARTS], refs[2 * PARTS :]
    w = gathered(ag)
    base = q[...]
    scale = 12.0 * rho[...]
    rows[...] = stack_of(w * scale, base * scale)
    pair = stack_of(w, base)
    gram = products(pair, pair)
    stats = jnp.concatenate([gram[16:, 16:], gram[:16, 16:], gram[:16, :16]], axis=1)
    forward_product(rows, 32, matrix, out, stats)


def pair_sum(rs, out):
    half = out.shape[0]
    for k in range(half):
        out[k] = rs[k] + rs[half + k]


def second_sum(cells, rs, ag, keep, stats_out, t_out, l_out):
    total = added(rs)
    rows = unfolded(total, 32)
    stats = tall(total[:, 1024:]) * (1.0 / cells)
    stats_out[...] = lanes([stats], 128)
    lower, t = orthonormal([block_of(stats, 1)], [[block_of(stats, 0)]], block_of(stats, 2))
    l_out[...] = lower
    t_out[...] = t
    v = fdot(t, rows)
    keep[...] = jnp.concatenate([v, rows[16:]], axis=0)
    copies(ag, v)


def third_pass(ag, left_rows, stats0, rho, *refs):
    matrix, (out, rows) = refs[: 2 * PARTS], refs[2 * PARTS :]
    v = gathered(ag)
    rows[...] = stack_of(v)
    gram = products(rows[...], left_rows[...])
    stats = lanes([gram[:, 16:], gram[:, :16], products(rows[...], rows[...]), stats0[:, :48]], 128)

    size = matrix[0].shape[0]
    step = 2 * TILE

    def cell_block(part, cb, carry):
        g0 = pl.multiple_of(cb * step, step)
        c0 = pl.multiple_of(part * size + g0, step)
        big = bdot(rows[...], matrix[2 * part][pl.ds(g0, step), :], NT)
        small = bdot(rows[:16, :], matrix[2 * part + 1][pl.ds(g0, step), :], NT)
        total = (big[:16] + big[16:] + small) * (12.0 * rho[0:1, pl.ds(c0, step)])
        for k in range(step // 128):
            piece = step // 128 * cb + k + part * (size // 128)
            out[piece, :16, :] = total[:, 128 * k : 128 * k + 128]
            out[piece, 16:, :] = stats
        return carry

    for part in range(PARTS):
        lax.fori_loop(0, size // step, functools.partial(cell_block, part), 0)


def third_sum(stations, rs, keep0, ag, base_out, t_out, l_out):
    total = added(rs)
    stats = total[16:] * (1.0 / stations)
    base = stats[:, 48:96]
    base_out[...] = lanes([base], 128)
    grams = [[block_of(base, 0)], [block_of(base, 1), block_of(base, 2)]]
    lower, t = orthonormal([block_of(stats, 0), block_of(stats, 1)], grams, block_of(stats, 2))
    l_out[...] = lower
    t_out[...] = t
    w = fdot(t, jnp.concatenate([total[:16], keep0[16:32, :], keep0[:16, :]], axis=0))
    copies(ag, w)


def fourth_pass(ag2, ag0, q, rho, t1, stats1, *refs):
    matrix, (right_out, own_out, out, rows) = refs[: 2 * PARTS], refs[2 * PARTS :]
    base = q[...]
    right = fdot(t1[...], jnp.concatenate([gathered(ag0), base], axis=0))
    right_out[...] = right
    w = gathered(ag2)
    rows[...] = stack_of(w * (12.0 * rho[...]))
    t_w, t_q = t1[:, :16], t1[:, 16:]
    qq, wq, ww = block_of(stats1, 0), block_of(stats1, 1), block_of(stats1, 2)
    with_q = fdot(t_w, wq) + fdot(t_q, qq)
    with_w = fdot(t_w, ww) + fdot(t_q, wq, NT)
    own_out[...] = lanes([with_q, fdot(with_w, t_w, NT) + fdot(with_q, t_q, NT)], 128)
    stats = products(stack_of(w), stack_of(base, right, w))
    forward_product(rows, 16, matrix, out, stats)


def fourth_sum(cells, rs, keep1, stats1, own1, ag, t_out, l_out):
    total = added(rs)
    stats = tall(total[:, 512:]) * (1.0 / cells)
    grams = [[block_of(stats1, 0)], [block_of(own1, 0), block_of(own1, 1)]]
    lower, t = orthonormal([block_of(stats, 0), block_of(stats, 1)], grams, block_of(stats, 2))
    l_out[...] = lower
    t_out[...] = t
    v = fdot(t, jnp.concatenate([unfolded(total, 16), keep1[16:, :], keep1[:16, :]], axis=0))
    copies(ag, v)


def last_stats(ag3, ag1, lb, ln, t2, left_out, out):
    before, now = lb[...], ln[...]
    left = fdot(t2[...], jnp.concatenate([gathered(ag1), before, now], axis=0))
    left_out[...] = left
    v = gathered(ag3)
    gram = products(stack_of(left, v), stack_of(before, now, left, v))
    copies(out, lanes([gram[:16, :48], gram[16:, :64]], 128))


def finish(stations, rs, base, ag3, lb, ln, left1, ag2, q, right1, t3, l1, l2, l3, rights, left_out, alphas, betas):
    stats = added(rs) * (1.0 / stations)
    grams = [
        [block_of(base, 0)],
        [block_of(base, 1), block_of(base, 2)],
        [block_of(stats, 0), block_of(stats, 1), block_of(stats, 2)],
    ]
    onto = [block_of(stats, 3), block_of(stats, 4), block_of(stats, 5)]
    lower, t = orthonormal(onto, grams, block_of(stats, 6))
    left_out[...] = fdot(t, jnp.concatenate([gathered(ag3), lb[...], ln[...], left1[...]], axis=0))
    rights[0] = right1[...]
    rights[1] = fdot(t3[...], jnp.concatenate([gathered(ag2), q[...], right1[...]], axis=0))
    alphas[0] = l1[...]
    alphas[1] = l3[...]
    betas[0] = l2[...]
    betas[1] = lower


def call(kernel, args, outs, scratch=(), limit=4, where=pltpu.VMEM):
    spec = pl.BlockSpec(memory_space=pltpu.VMEM)
    return pl.pallas_call(
        kernel,
        out_shape=tuple(outs),
        in_specs=[pl.BlockSpec(memory_space=where)] * len(args),
        out_specs=tuple(spec for _ in outs),
        scratch_shapes=list(scratch),
        compiler_params=pltpu.CompilerParams(vmem_limit_bytes=limit * 2**20),
    )(*args)


def f32(*shape):
    return jax.ShapeDtypeStruct(shape, F32)


def exchange(value, axis, groups=None):
    return lax.all_to_all(value, axis, split_axis=0, concat_axis=0, tiled=True, axis_index_groups=groups)


def body(station_plane, station_height, cell_plane, cell_depth, cell_density, left_before, left_now, right_before):
    n_s, n_c = left_now.shape[1], right_before.shape[1]
    n_sta, n_cel = lax.axis_size("sta"), lax.axis_size("cel")
    stations, cells = n_s * n_sta, n_c * n_cel
    cp, sp = n_c // n_sta, n_s // n_cel
    small = f32(16, 16)

    inputs = (
        station_plane,
        station_height.reshape(1, n_s),
        cell_plane,
        cell_depth.reshape(1, n_c),
        cell_density.reshape(1, n_c),
        left_before,
        left_now,
        right_before,
    )
    sp_v, sh_v, cp_v, cd_v, rho, lb, ln, q = call(
        fetch,
        inputs,
        [pltpu.VMEM(v.shape, v.dtype) for v in inputs],
        [pltpu.SemaphoreType.DMA((len(inputs),))],
        limit=LARGE,
        where=pltpu.HBM,
    )
    *matrix, rs0, left_rows, stats0 = call(
        first_pass,
        (sp_v, sh_v, cp_v, cd_v, rho, lb, ln),
        (
            *[pltpu.VMEM((n_c // PARTS, n_s), BF16)] * (2 * PARTS),
            f32(n_sta, 32, cp),
            pltpu.VMEM((64, n_s), BF16),
            f32(16, 128),
        ),
        [
            pltpu.VMEM((8, n_s), F32),
            pltpu.VMEM((TILE, 128), F32),
            pltpu.VMEM((TILE, 16), BF16),
            pltpu.VMEM((16, n_s), BF16),
            pltpu.VMEM((TILE, n_s), F32),
        ],
        limit=10,
    )
    ag0, keep0 = call(first_sum, (exchange(rs0, "sta"),), (f32(n_sta, 16, cp), f32(32, cp)))
    ag0 = exchange(ag0, "sta")
    (rs1,) = call(second_pass, (ag0, q, rho, *matrix), (f32(n_cel, 8, 1152),), [pltpu.VMEM((64, n_c), BF16)])
    half = n_cel // 2
    across = [[k, half + k] for k in range(half)]
    along = [[half * side + k for k in range(half)] for side in range(2)]
    (rs1,) = call(pair_sum, (exchange(rs1, "cel", across),), (f32(half, 8, 1152),))
    ag1, keep1, stats1, t1, l1 = call(
        lambda *refs: second_sum(cells, *refs),
        (exchange(rs1, "cel", along),),
        (f32(n_cel, 16, sp), f32(32, sp), f32(16, 128), f32(16, 32), small),
    )
    ag1 = exchange(ag1, "cel")
    (rs2,) = call(third_pass, (ag1, left_rows, stats0, rho, *matrix), (f32(n_sta, 32, cp),), [pltpu.VMEM((32, n_s), BF16)])
    ag2, base2, t2, l2 = call(
        lambda *refs: third_sum(stations, *refs),
        (exchange(rs2, "sta"), keep0),
        (f32(n_sta, 16, cp), f32(16, 128), f32(16, 48), small),
    )
    ag2 = exchange(ag2, "sta")
    right1, own1, rs3 = call(
        fourth_pass,
        (ag2, ag0, q, rho, t1, stats1, *matrix),
        (f32(16, n_c), f32(16, 128), f32(n_cel, 8, 640)),
        [pltpu.VMEM((32, n_c), BF16)],
    )
    ag3, t3, l3 = call(
        lambda *refs: fourth_sum(cells, *refs),
        (exchange(rs3, "cel"), keep1, stats1, own1),
        (f32(n_cel, 16, sp), f32(16, 48), small),
    )
    ag3 = exchange(ag3, "cel")
    left1, rs4 = call(last_stats, (ag3, ag1, lb, ln, t2), (f32(16, n_s), f32(n_sta, 16, 128)))
    rights, left2, alphas, betas = call(
        lambda *refs: finish(stations, *refs),
        (exchange(rs4, "sta"), base2, ag3, lb, ln, left1, ag2, q, right1, t3, l1, l2, l3),
        (f32(2, 16, n_c), f32(16, n_s), f32(2, 16, 16), f32(2, 16, 16)),
    )
    return rights, left2, alphas, betas


def solution(mesh):
    in_specs = (
        P(None, "sta"),
        P("sta"),
        P(None, "cel"),
        P("cel"),
        P("cel"),
        P(None, "sta"),
        P(None, "sta"),
        P(None, "cel"),
    )
    out_specs = (P(None, None, "cel"), P(None, "sta"), P(), P())
    return jax.shard_map(body, mesh=mesh, in_specs=in_specs, out_specs=out_specs, check_vma=False)
```

```python
import functools

import jax
import jax.numpy as jnp
from jax import lax
from jax.experimental import pallas as pl
from jax.experimental.pallas import tpu as pltpu
from jax.sharding import PartitionSpec as P

F32 = jnp.float32
BF16 = jnp.bfloat16
HIGH = lax.Precision.HIGHEST
TILE = 256
NN = (((1,), (0,)), ((), ()))
NT = (((1,), (1,)), ((), ()))


def fdot(a, b, dims=NN):
    return lax.dot_general(a, b, dims, precision=HIGH, preferred_element_type=F32)


def bdot(a, b, dims=NN):
    return lax.dot_general(a, b, dims, preferred_element_type=F32)


def halves(x):
    hi = x.astype(BF16)
    lo = (x - hi.astype(F32)).astype(BF16)
    return hi, lo


def lanes(blocks, width):
    used = sum(b.shape[1] for b in blocks)
    rows = blocks[0].shape[0]
    return jnp.concatenate([*blocks, jnp.zeros((rows, width - used), F32)], axis=1)


def block_of(stats, index):
    return stats[:, 16 * index : 16 * index + 16]


def wide(stats):
    return lanes([stats[:8], stats[8:]], 128)


def tall(tile):
    return jnp.concatenate([tile[:, :48], tile[:, 48:96]], axis=0)


def unfolded(message, count):
    return jnp.concatenate([message[:, 256 * k : 256 * k + 256] for k in range(count // 8)], axis=0)


def factor(gram):
    size = gram.shape[0]
    row = lax.broadcasted_iota(jnp.int32, (size, 2 * size), 0)
    lane = lax.broadcasted_iota(jnp.int32, (size, 2 * size), 1)
    work = jnp.concatenate([gram, jnp.zeros_like(gram)], axis=1)
    work = work + jnp.where(lane == row + size, 1.0, 0.0)
    lower = jnp.zeros_like(work)
    for k in range(size):
        column = jnp.broadcast_to(work[:, k : k + 1], work.shape)
        pivot = column[k : k + 1, :]
        r = lax.rsqrt(pivot)
        r = r * (1.5 - 0.5 * pivot * r * r)
        column = column * r
        lower = jnp.where((lane == k) & (row >= k), column, lower)
        line = work[k : k + 1, :] * r
        work = jnp.where(row == k, line, work - jnp.where(row > k, column, 0.0) * line)
    return lower[:, :size], work[:, size:]


def tdot(t, x):
    t_hi, t_lo = halves(t)
    x_hi, x_lo = halves(x)
    size = t.shape[0]
    big = bdot(jnp.concatenate([t_hi, t_lo], axis=0), x_hi)
    return big[:size] + (big[size:] + bdot(t_hi, x_lo))


def orthonormal(onto, basis, own):
    count = len(onto)
    gram = own
    for l in range(count):
        part = -2.0 * onto[l]
        for m in range(count):
            if m >= l:
                part = part + fdot(onto[m], basis[m][l])
            else:
                part = part + fdot(onto[m], basis[l][m], NT)
        gram = gram + fdot(part, onto[l], NT)
    lower, inv = factor(gram)
    return lower, jnp.concatenate([inv] + [-fdot(inv, c) for c in onto], axis=1)


def added(ref):
    total = ref[0]
    for k in range(1, ref.shape[0]):
        total = total + ref[k]
    return total


def copies(ref, value):
    for k in range(ref.shape[0]):
        ref[k] = value


def gathered(ref):
    return jnp.concatenate([ref[k] for k in range(ref.shape[0])], axis=1)


def stack_of(*values):
    parts = [halves(v) for v in values]
    return jnp.concatenate([p[0] for p in parts] + [p[1] for p in parts], axis=0)


def products(x, y):
    m, k = x.shape[0] // 2, y.shape[0] // 2
    full = bdot(x, y, NT)
    return full[:m, :k] + (full[:m, k:] + full[m:, :k]) + full[m:, k:]


PARTS = 2
LARGE = 62


def pieces(x):
    first = x.astype(BF16).astype(F32)
    second = (x - first).astype(BF16).astype(F32)
    return [first, second, x - first - second]


def fetch(*refs):
    count = len(refs) // 2
    sems = refs[-1]
    moves = [pltpu.make_async_copy(refs[k], refs[count + k], sems.at[k]) for k in range(count)]
    for move in moves:
        move.start()
    for move in moves:
        move.wait()


def first_pass(sp_v, sh_v, cp_v, cd_v, rho_v, lb_v, ln_v, *refs):
    matrix, refs = refs[: 2 * PARTS], refs[2 * PARTS :]
    out, rows, stats_out, sz_v, czb, a_ref, b_ref, square = refs
    n_s, n_c = sp_v.shape[1], cp_v.shape[1]

    sx, sy = sp_v[0:1, :].astype(F32), sp_v[1:2, :].astype(F32)
    sz = sh_v[...].astype(F32) + 0.5
    sz_v[...] = jnp.broadcast_to(sz, sz_v.shape)
    one, zero = jnp.ones_like(sx), jnp.zeros_like(sx)
    b_rows = pieces(sx * sx + sy * sy + sz * sz) + [one, one, one, -2.0 * sx, -2.0 * sy, 2.0 * sz] + [zero] * 7
    b_ref[...] = jnp.concatenate(b_rows, axis=0).astype(BF16)

    rows[...] = stack_of(ln_v[...], lb_v[...])
    gram = products(rows[...], rows[...])
    stats_out[...] = lanes([gram[16:, 16:], gram[:16, 16:], gram[:16, :16]], 128)

    def prepare(c0):
        for half in range(2):
            here = pl.ds(pl.multiple_of(c0 + 128 * half, 128), 128)
            put = slice(128 * half, 128 * half + 128)
            cx, cy = cp_v[0:1, here].astype(F32), cp_v[1:2, here].astype(F32)
            cz = cd_v[0:1, here].astype(F32)
            unit, none = jnp.ones_like(cx), jnp.zeros_like(cx)
            a_rows = [unit, unit, unit] + pieces(cx * cx + cy * cy + cz * cz) + [cx, cy, cz] + [none] * 7
            turned = jnp.transpose(jnp.concatenate(a_rows, axis=0))
            a_ref[put, :] = turned.astype(BF16)
            czb[put, :] = jnp.broadcast_to(turned[:, 8:9], (128, 128))

    def cell_block(part, cb, carry):
        hi_ref, lo_ref = matrix[2 * part], matrix[2 * part + 1]
        g0 = pl.multiple_of(cb * TILE, TILE)
        c0 = pl.multiple_of(part * (n_c // PARTS) + g0, TILE)

        def station_block(sb, inner):
            for half in range(2):
                here = pl.ds(pl.multiple_of(sb * 2 * TILE + half * TILE, TILE), TILE)
                height = sz_v[:, here]
                for r0 in range(0, TILE, 8):
                    dz = height + jnp.concatenate([czb[r0 : r0 + 8, :]] * 2, axis=1)
                    inv = lax.rsqrt(square[r0 : r0 + 8, here])
                    inv2 = inv * inv
                    g = (dz * dz * inv2 - (1.0 / 3.0)) * (inv2 * inv)
                    where = pl.ds(pl.multiple_of(g0 + r0, 8), 8)
                    hi_ref[where, here] = g.astype(BF16)
                    lo_ref[where, here] = (g - hi_ref[where, here].astype(F32)).astype(BF16)
            return inner

        lax.fori_loop(0, n_s // (2 * TILE), station_block, 0)
        prepare(jnp.minimum(c0 + TILE, n_c - TILE))
        big = bdot(rows[...], hi_ref[pl.ds(g0, TILE), :], NT)
        small = bdot(rows[:32, :], lo_ref[pl.ds(g0, TILE), :], NT)
        total = (big[:32] + big[32:] + small) * (12.0 * rho_v[0:1, pl.ds(c0, TILE)])
        for k in range(2):
            piece = 2 * cb + k + part * (n_c // PARTS // 128)
            out[piece] = total[:, 128 * k : 128 * k + 128]
        square[...] = bdot(a_ref[...], b_ref[...])
        return carry

    prepare(0)
    square[...] = bdot(a_ref[...], b_ref[...])
    for part in range(PARTS):
        lax.fori_loop(0, n_c // PARTS // TILE, functools.partial(cell_block, part), 0)


def first_sum(rs, ag, keep):
    total = added(rs)
    keep[...] = total
    copies(ag, total[:16])


def forward_product(rows, count, matrix, out, stats):
    step = 4 * TILE
    size = matrix[0].shape[0]
    tile = wide(stats)

    def station_block(sb, carry):
        s0 = pl.multiple_of(sb * step, step)
        total = jnp.zeros((count, step), F32)
        for part in range(PARTS):
            own = slice(part * size, part * size + size)
            big = bdot(rows[:, own], matrix[2 * part][:, pl.ds(s0, step)])
            small = bdot(rows[:count, own], matrix[2 * part + 1][:, pl.ds(s0, step)])
            total = total + (big[:count] + big[count:] + small)
        for k in range(step // TILE):
            piece = sb * (step // TILE) + k
            for r in range(count // 8):
                out[piece, :, 256 * r : 256 * r + 256] = total[8 * r : 8 * r + 8, TILE * k : TILE * k + TILE]
            out[piece, :, 32 * count :] = tile
        return carry

    lax.fori_loop(0, matrix[0].shape[1] // step, station_block, 0)


def second_pass(ag, q, rho, *refs):
    matrix, (out, rows) = refs[: 2 * PARTS], refs[2 * PARTS :]
    w = gathered(ag)
    base = q[...]
    scale = 12.0 * rho[...]
    rows[...] = stack_of(w * scale, base * scale)
    pair = stack_of(w, base)
    gram = products(pair, pair)
    stats = jnp.concatenate([gram[16:, 16:], gram[:16, 16:], gram[:16, :16]], axis=1)
    forward_product(rows, 32, matrix, out, stats)


def second_sum(cells, rs, ag, keep, stats_out, t_out, l_out):
    total = added(rs)
    rows = unfolded(total, 32)
    stats = tall(total[:, 1024:]) * (1.0 / cells)
    stats_out[...] = lanes([stats], 128)
    lower, t = orthonormal([block_of(stats, 1)], [[block_of(stats, 0)]], block_of(stats, 2))
    l_out[...] = lower
    t_out[...] = t
    v = fdot(t, rows)
    keep[...] = jnp.concatenate([v, rows[16:]], axis=0)
    copies(ag, v)


def third_pass(ag, left_rows, stats0, rho, *refs):
    matrix, (out, rows) = refs[: 2 * PARTS], refs[2 * PARTS :]
    v = gathered(ag)
    rows[...] = stack_of(v)
    gram = products(rows[...], left_rows[...])
    stats = lanes([gram[:, 16:], gram[:, :16], products(rows[...], rows[...]), stats0[:, :48]], 128)

    size = matrix[0].shape[0]
    step = 2 * TILE

    def cell_block(part, cb, carry):
        g0 = pl.multiple_of(cb * step, step)
        c0 = pl.multiple_of(part * size + g0, step)
        big = bdot(rows[...], matrix[2 * part][pl.ds(g0, step), :], NT)
        small = bdot(rows[:16, :], matrix[2 * part + 1][pl.ds(g0, step), :], NT)
        total = (big[:16] + big[16:] + small) * (12.0 * rho[0:1, pl.ds(c0, step)])
        for k in range(step // 128):
            piece = step // 128 * cb + k + part * (size // 128)
            out[piece, :16, :] = total[:, 128 * k : 128 * k + 128]
            out[piece, 16:, :] = stats
        return carry

    for part in range(PARTS):
        lax.fori_loop(0, size // step, functools.partial(cell_block, part), 0)


def third_sum(stations, rs, keep0, ag, base_out, t_out, l_out):
    total = added(rs)
    stats = total[16:] * (1.0 / stations)
    base = stats[:, 48:96]
    base_out[...] = lanes([base], 128)
    grams = [[block_of(base, 0)], [block_of(base, 1), block_of(base, 2)]]
    lower, t = orthonormal([block_of(stats, 0), block_of(stats, 1)], grams, block_of(stats, 2))
    l_out[...] = lower
    t_out[...] = t
    w = fdot(t, jnp.concatenate([total[:16], keep0[16:32, :], keep0[:16, :]], axis=0))
    copies(ag, w)


def fourth_pass(ag2, ag0, q, rho, t1, stats1, *refs):
    matrix, (right_out, own_out, out, rows) = refs[: 2 * PARTS], refs[2 * PARTS :]
    base = q[...]
    right = tdot(t1[...], jnp.concatenate([gathered(ag0), base], axis=0))
    right_out[...] = right
    w = gathered(ag2)
    rows[...] = stack_of(w * (12.0 * rho[...]))
    t_w, t_q = t1[:, :16], t1[:, 16:]
    qq, wq, ww = block_of(stats1, 0), block_of(stats1, 1), block_of(stats1, 2)
    with_q = fdot(t_w, wq) + fdot(t_q, qq)
    with_w = fdot(t_w, ww) + fdot(t_q, wq, NT)
    own_out[...] = lanes([with_q, fdot(with_w, t_w, NT) + fdot(with_q, t_q, NT)], 128)
    stats = products(stack_of(w), stack_of(base, right, w))
    forward_product(rows, 16, matrix, out, stats)


def fourth_sum(cells, rs, keep1, stats1, own1, ag, t_out, l_out):
    total = added(rs)
    stats = tall(total[:, 512:]) * (1.0 / cells)
    grams = [[block_of(stats1, 0)], [block_of(own1, 0), block_of(own1, 1)]]
    lower, t = orthonormal([block_of(stats, 0), block_of(stats, 1)], grams, block_of(stats, 2))
    l_out[...] = lower
    t_out[...] = t
    v = fdot(t, jnp.concatenate([unfolded(total, 16), keep1[16:, :], keep1[:16, :]], axis=0))
    copies(ag, v)


def last_stats(ag3, ag1, lb, ln, t2, left_out, out):
    before, now = lb[...], ln[...]
    left = tdot(t2[...], jnp.concatenate([gathered(ag1), before, now], axis=0))
    left_out[...] = left
    v = gathered(ag3)
    gram = products(stack_of(left, v), stack_of(before, now, left, v))
    copies(out, lanes([gram[:16, :48], gram[16:, :64]], 128))


def finish(stations, rs, base, ag3, lb, ln, left1, ag2, q, right1, t3, l1, l2, l3, rights, left_out, alphas, betas):
    stats = added(rs) * (1.0 / stations)
    grams = [
        [block_of(base, 0)],
        [block_of(base, 1), block_of(base, 2)],
        [block_of(stats, 0), block_of(stats, 1), block_of(stats, 2)],
    ]
    onto = [block_of(stats, 3), block_of(stats, 4), block_of(stats, 5)]
    lower, t = orthonormal(onto, grams, block_of(stats, 6))
    left_out[...] = tdot(t, jnp.concatenate([gathered(ag3), lb[...], ln[...], left1[...]], axis=0))
    rights[0] = right1[...]
    rights[1] = tdot(t3[...], jnp.concatenate([gathered(ag2), q[...], right1[...]], axis=0))
    alphas[0] = l1[...]
    alphas[1] = l3[...]
    betas[0] = l2[...]
    betas[1] = lower


def call(kernel, args, outs, scratch=(), limit=4, where=pltpu.VMEM):
    spec = pl.BlockSpec(memory_space=pltpu.VMEM)
    return pl.pallas_call(
        kernel,
        out_shape=tuple(outs),
        in_specs=[pl.BlockSpec(memory_space=where)] * len(args),
        out_specs=tuple(spec for _ in outs),
        scratch_shapes=list(scratch),
        compiler_params=pltpu.CompilerParams(vmem_limit_bytes=limit * 2**20),
    )(*args)


def f32(*shape):
    return jax.ShapeDtypeStruct(shape, F32)


def exchange(value, axis):
    return lax.all_to_all(value, axis, split_axis=0, concat_axis=0, tiled=True)


def body(station_plane, station_height, cell_plane, cell_depth, cell_density, left_before, left_now, right_before):
    n_s, n_c = left_now.shape[1], right_before.shape[1]
    n_sta, n_cel = lax.axis_size("sta"), lax.axis_size("cel")
    stations, cells = n_s * n_sta, n_c * n_cel
    cp, sp = n_c // n_sta, n_s // n_cel
    small = f32(16, 16)

    inputs = (
        station_plane,
        station_height.reshape(1, n_s),
        cell_plane,
        cell_depth.reshape(1, n_c),
        cell_density.reshape(1, n_c),
        left_before,
        left_now,
        right_before,
    )
    sp_v, sh_v, cp_v, cd_v, rho, lb, ln, q = call(
        fetch,
        inputs,
        [pltpu.VMEM(v.shape, v.dtype) for v in inputs],
        [pltpu.SemaphoreType.DMA((len(inputs),))],
        limit=LARGE,
        where=pltpu.HBM,
    )
    *matrix, rs0, left_rows, stats0 = call(
        first_pass,
        (sp_v, sh_v, cp_v, cd_v, rho, lb, ln),
        (
            *[pltpu.VMEM((n_c // PARTS, n_s), BF16)] * (2 * PARTS),
            f32(n_sta, 32, cp),
            pltpu.VMEM((64, n_s), BF16),
            f32(16, 128),
        ),
        [
            pltpu.VMEM((8, n_s), F32),
            pltpu.VMEM((TILE, 128), F32),
            pltpu.VMEM((TILE, 16), BF16),
            pltpu.VMEM((16, n_s), BF16),
            pltpu.VMEM((TILE, n_s), F32),
        ],
        limit=10,
    )
    ag0, keep0 = call(first_sum, (exchange(rs0, "sta"),), (f32(n_sta, 16, cp), f32(32, cp)))
    ag0 = exchange(ag0, "sta")
    (rs1,) = call(second_pass, (ag0, q, rho, *matrix), (f32(n_cel, 8, 1152),), [pltpu.VMEM((64, n_c), BF16)])
    ag1, keep1, stats1, t1, l1 = call(
        lambda *refs: second_sum(cells, *refs),
        (exchange(rs1, "cel"),),
        (f32(n_cel, 16, sp), f32(32, sp), f32(16, 128), f32(16, 32), small),
    )
    ag1 = exchange(ag1, "cel")
    (rs2,) = call(third_pass, (ag1, left_rows, stats0, rho, *matrix), (f32(n_sta, 32, cp),), [pltpu.VMEM((32, n_s), BF16)])
    ag2, base2, t2, l2 = call(
        lambda *refs: third_sum(stations, *refs),
        (exchange(rs2, "sta"), keep0),
        (f32(n_sta, 16, cp), f32(16, 128), f32(16, 48), small),
    )
    ag2 = exchange(ag2, "sta")
    right1, own1, rs3 = call(
        fourth_pass,
        (ag2, ag0, q, rho, t1, stats1, *matrix),
        (f32(16, n_c), f32(16, 128), f32(n_cel, 8, 640)),
        [pltpu.VMEM((32, n_c), BF16)],
    )
    ag3, t3, l3 = call(
        lambda *refs: fourth_sum(cells, *refs),
        (exchange(rs3, "cel"), keep1, stats1, own1),
        (f32(n_cel, 16, sp), f32(16, 48), small),
    )
    ag3 = exchange(ag3, "cel")
    left1, rs4 = call(last_stats, (ag3, ag1, lb, ln, t2), (f32(16, n_s), f32(n_sta, 16, 128)))
    rights, left2, alphas, betas = call(
        lambda *refs: finish(stations, *refs),
        (exchange(rs4, "sta"), base2, ag3, lb, ln, left1, ag2, q, right1, t3, l1, l2, l3),
        (f32(2, 16, n_c), f32(16, n_s), f32(2, 16, 16), f32(2, 16, 16)),
    )
    return rights, left2, alphas, betas


def solution(mesh):
    in_specs = (
        P(None, "sta"),
        P("sta"),
        P(None, "cel"),
        P("cel"),
        P("cel"),
        P(None, "sta"),
        P(None, "sta"),
        P(None, "cel"),
    )
    out_specs = (P(None, None, "cel"), P(None, "sta"), P(), P())
    return jax.shard_map(body, mesh=mesh, in_specs=in_specs, out_specs=out_specs, check_vma=False)
```

```python
import functools

import jax
import jax.numpy as jnp
from jax import lax
from jax.experimental import pallas as pl
from jax.experimental.pallas import tpu as pltpu
from jax.sharding import PartitionSpec as P

F32 = jnp.float32
BF16 = jnp.bfloat16
HIGH = lax.Precision.HIGHEST
TILE = 256
NN = (((1,), (0,)), ((), ()))
NT = (((1,), (1,)), ((), ()))


def fdot(a, b, dims=NN):
    return lax.dot_general(a, b, dims, precision=HIGH, preferred_element_type=F32)


def bdot(a, b, dims=NN):
    return lax.dot_general(a, b, dims, preferred_element_type=F32)


def halves(x):
    hi = x.astype(BF16)
    lo = (x - hi.astype(F32)).astype(BF16)
    return hi, lo


def lanes(blocks, width):
    used = sum(b.shape[1] for b in blocks)
    rows = blocks[0].shape[0]
    return jnp.concatenate([*blocks, jnp.zeros((rows, width - used), F32)], axis=1)


def block_of(stats, index):
    return stats[:, 16 * index : 16 * index + 16]


def wide(stats):
    return lanes([stats[:8], stats[8:]], 128)


def tall(tile):
    return jnp.concatenate([tile[:, :48], tile[:, 48:96]], axis=0)


def unfolded(message, count):
    return jnp.concatenate([message[:, 256 * k : 256 * k + 256] for k in range(count // 8)], axis=0)


def factor(gram):
    size = gram.shape[0]
    shape = (size, 128)
    row = lax.broadcasted_iota(jnp.int32, shape, 0)
    lane = lax.broadcasted_iota(jnp.int32, shape, 1)
    columns = [jnp.broadcast_to(gram[:, k : k + 1], shape) for k in range(size)]
    inv = jnp.where(lane == row, 1.0, 0.0)
    lower = jnp.zeros(shape, F32)
    for k in range(size):
        pivot = columns[k][k : k + 1, :]
        r = lax.rsqrt(pivot)
        r = r * (1.5 - 0.5 * pivot * r * r)
        column = columns[k] * r
        for j in range(k + 1, size):
            columns[j] = columns[j] - column * column[j : j + 1, :]
        lower = jnp.where((lane == k) & (row >= k), column, lower)
        line = inv[k : k + 1, :] * r
        inv = jnp.where(row == k, line, inv - jnp.where(row > k, column, 0.0) * line)
    return lower[:, :size], inv[:, :size]


def orthonormal(onto, basis, own):
    count = len(onto)
    coef = jnp.concatenate(onto, axis=1)
    lines = []
    for m in range(count):
        line = [*basis[m][:m], 0.5 * basis[m][m]] + [jnp.zeros_like(own)] * (count - 1 - m)
        lines.append(jnp.concatenate(line, axis=1))
    part = fdot(coef, jnp.concatenate(lines, axis=0)) - coef
    gram = own + (fdot(part, coef, NT) + fdot(coef, part, NT))
    lower, inv = factor(gram)
    return lower, jnp.concatenate([inv, -fdot(inv, coef)], axis=1)


def tdot(t, x):
    t_hi, t_lo = halves(t)
    x_hi, x_lo = halves(x)
    size = t.shape[0]
    big = bdot(jnp.concatenate([t_hi, t_lo], axis=0), x_hi)
    return big[:size] + (big[size:] + bdot(t_hi, x_lo))


def added(ref):
    total = ref[0]
    for k in range(1, ref.shape[0]):
        total = total + ref[k]
    return total


def copies(ref, value):
    for k in range(ref.shape[0]):
        ref[k] = value


def gathered(ref):
    return jnp.concatenate([ref[k] for k in range(ref.shape[0])], axis=1)


def stack_of(*values):
    parts = [halves(v) for v in values]
    return jnp.concatenate([p[0] for p in parts] + [p[1] for p in parts], axis=0)


def products(x, y):
    m, k = x.shape[0] // 2, y.shape[0] // 2
    full = bdot(x, y, NT)
    return full[:m, :k] + (full[:m, k:] + full[m:, :k]) + full[m:, k:]


PARTS = 2
LARGE = 62


def pieces(x):
    first = x.astype(BF16).astype(F32)
    second = (x - first).astype(BF16).astype(F32)
    return [first, second, x - first - second]


def fetch(*refs):
    count = len(refs) // 2
    sems = refs[-1]
    moves = [pltpu.make_async_copy(refs[k], refs[count + k], sems.at[k]) for k in range(count)]
    for move in moves:
        move.start()
    for move in moves:
        move.wait()


def first_pass(sp_v, sh_v, cp_v, cd_v, rho_v, lb_v, ln_v, *refs):
    matrix, refs = refs[: 2 * PARTS], refs[2 * PARTS :]
    out, rows, stats_out, sz_v, czb, a_ref, b_ref, square = refs
    n_s, n_c = sp_v.shape[1], cp_v.shape[1]

    sx, sy = sp_v[0:1, :].astype(F32), sp_v[1:2, :].astype(F32)
    sz = sh_v[...].astype(F32) + 0.5
    sz_v[...] = jnp.broadcast_to(sz, sz_v.shape)
    one, zero = jnp.ones_like(sx), jnp.zeros_like(sx)
    b_rows = pieces(sx * sx + sy * sy + sz * sz) + [one, one, one, -2.0 * sx, -2.0 * sy, 2.0 * sz] + [zero] * 7
    b_ref[...] = jnp.concatenate(b_rows, axis=0).astype(BF16)

    rows[...] = stack_of(ln_v[...], lb_v[...])
    gram = products(rows[...], rows[...])
    stats_out[...] = lanes([gram[16:, 16:], gram[:16, 16:], gram[:16, :16]], 128)

    def prepare(c0):
        for half in range(2):
            here = pl.ds(pl.multiple_of(c0 + 128 * half, 128), 128)
            put = slice(128 * half, 128 * half + 128)
            cx, cy = cp_v[0:1, here].astype(F32), cp_v[1:2, here].astype(F32)
            cz = cd_v[0:1, here].astype(F32)
            unit, none = jnp.ones_like(cx), jnp.zeros_like(cx)
            a_rows = [unit, unit, unit] + pieces(cx * cx + cy * cy + cz * cz) + [cx, cy, cz] + [none] * 7
            turned = jnp.transpose(jnp.concatenate(a_rows, axis=0))
            a_ref[put, :] = turned.astype(BF16)
            czb[put, :] = jnp.broadcast_to(turned[:, 8:9], (128, 128))

    def cell_block(part, cb, carry):
        hi_ref, lo_ref = matrix[2 * part], matrix[2 * part + 1]
        g0 = pl.multiple_of(cb * TILE, TILE)
        c0 = pl.multiple_of(part * (n_c // PARTS) + g0, TILE)

        def station_block(sb, inner):
            for half in range(2):
                here = pl.ds(pl.multiple_of(sb * 2 * TILE + half * TILE, TILE), TILE)
                height = sz_v[:, here]
                for r0 in range(0, TILE, 8):
                    dz = height + jnp.concatenate([czb[r0 : r0 + 8, :]] * 2, axis=1)
                    inv = lax.rsqrt(square[r0 : r0 + 8, here])
                    inv2 = inv * inv
                    g = (dz * dz * inv2 - (1.0 / 3.0)) * (inv2 * inv)
                    where = pl.ds(pl.multiple_of(g0 + r0, 8), 8)
                    hi_ref[where, here] = g.astype(BF16)
                    lo_ref[where, here] = (g - hi_ref[where, here].astype(F32)).astype(BF16)
            return inner

        lax.fori_loop(0, n_s // (2 * TILE), station_block, 0)
        prepare(jnp.minimum(c0 + TILE, n_c - TILE))
        big = bdot(rows[...], hi_ref[pl.ds(g0, TILE), :], NT)
        small = bdot(rows[:32, :], lo_ref[pl.ds(g0, TILE), :], NT)
        total = (big[:32] + big[32:] + small) * (12.0 * rho_v[0:1, pl.ds(c0, TILE)])
        for k in range(2):
            piece = 2 * cb + k + part * (n_c // PARTS // 128)
            out[piece] = total[:, 128 * k : 128 * k + 128]
        square[...] = bdot(a_ref[...], b_ref[...])
        return carry

    prepare(0)
    square[...] = bdot(a_ref[...], b_ref[...])
    for part in range(PARTS):
        lax.fori_loop(0, n_c // PARTS // TILE, functools.partial(cell_block, part), 0)


def first_sum(rs, ag, keep):
    total = added(rs)
    keep[...] = total
    copies(ag, total[:16])


def forward_product(rows, count, matrix, out, stats):
    step = 4 * TILE
    size = matrix[0].shape[0]
    tile = wide(stats)

    def station_block(sb, carry):
        s0 = pl.multiple_of(sb * step, step)
        total = jnp.zeros((count, step), F32)
        for part in range(PARTS):
            own = slice(part * size, part * size + size)
            big = bdot(rows[:, own], matrix[2 * part][:, pl.ds(s0, step)])
            small = bdot(rows[:count, own], matrix[2 * part + 1][:, pl.ds(s0, step)])
            total = total + (big[:count] + big[count:] + small)
        for k in range(step // TILE):
            piece = sb * (step // TILE) + k
            for r in range(count // 8):
                out[piece, :, 256 * r : 256 * r + 256] = total[8 * r : 8 * r + 8, TILE * k : TILE * k + TILE]
            out[piece, :, 32 * count :] = tile
        return carry

    lax.fori_loop(0, matrix[0].shape[1] // step, station_block, 0)


def second_pass(ag, q, rho, *refs):
    matrix, (out, rows) = refs[: 2 * PARTS], refs[2 * PARTS :]
    w = gathered(ag)
    base = q[...]
    scale = 12.0 * rho[...]
    rows[...] = stack_of(w * scale, base * scale)
    pair = stack_of(w, base)
    gram = products(pair, pair)
    stats = jnp.concatenate([gram[16:, 16:], gram[:16, 16:], gram[:16, :16]], axis=1)
    forward_product(rows, 32, matrix, out, stats)


def second_sum(cells, rs, ag, keep, stats_out, t_out, l_out):
    total = added(rs)
    rows = unfolded(total, 32)
    stats = tall(total[:, 1024:]) * (1.0 / cells)
    stats_out[...] = lanes([stats], 128)
    lower, t = orthonormal([block_of(stats, 1)], [[block_of(stats, 0)]], block_of(stats, 2))
    l_out[...] = lower
    t_out[...] = t
    v = fdot(t, rows)
    keep[...] = jnp.concatenate([v, rows[16:]], axis=0)
    copies(ag, v)


def third_pass(ag, left_rows, stats0, rho, *refs):
    matrix, (out, rows) = refs[: 2 * PARTS], refs[2 * PARTS :]
    v = gathered(ag)
    rows[...] = stack_of(v)
    gram = products(rows[...], left_rows[...])
    stats = lanes([gram[:, 16:], gram[:, :16], products(rows[...], rows[...]), stats0[:, :48]], 128)

    size = matrix[0].shape[0]
    step = 2 * TILE

    def cell_block(part, cb, carry):
        g0 = pl.multiple_of(cb * step, step)
        c0 = pl.multiple_of(part * size + g0, step)
        big = bdot(rows[...], matrix[2 * part][pl.ds(g0, step), :], NT)
        small = bdot(rows[:16, :], matrix[2 * part + 1][pl.ds(g0, step), :], NT)
        total = (big[:16] + big[16:] + small) * (12.0 * rho[0:1, pl.ds(c0, step)])
        for k in range(step // 128):
            piece = step // 128 * cb + k + part * (size // 128)
            out[piece, :16, :] = total[:, 128 * k : 128 * k + 128]
            out[piece, 16:, :] = stats
        return carry

    for part in range(PARTS):
        lax.fori_loop(0, size // step, functools.partial(cell_block, part), 0)


def third_sum(stations, rs, keep0, ag, base_out, t_out, l_out):
    total = added(rs)
    stats = total[16:] * (1.0 / stations)
    base = stats[:, 48:96]
    base_out[...] = lanes([base], 128)
    grams = [[block_of(base, 0)], [block_of(base, 1), block_of(base, 2)]]
    lower, t = orthonormal([block_of(stats, 0), block_of(stats, 1)], grams, block_of(stats, 2))
    l_out[...] = lower
    t_out[...] = t
    w = fdot(t, jnp.concatenate([total[:16], keep0[16:32, :], keep0[:16, :]], axis=0))
    copies(ag, w)


def fourth_pass(ag2, ag0, q, rho, t1, stats1, *refs):
    matrix, (right_out, own_out, out, rows) = refs[: 2 * PARTS], refs[2 * PARTS :]
    base = q[...]
    right = tdot(t1[...], jnp.concatenate([gathered(ag0), base], axis=0))
    right_out[...] = right
    w = gathered(ag2)
    rows[...] = stack_of(w * (12.0 * rho[...]))
    t_w, t_q = t1[:, :16], t1[:, 16:]
    qq, wq, ww = block_of(stats1, 0), block_of(stats1, 1), block_of(stats1, 2)
    with_q = fdot(t_w, wq) + fdot(t_q, qq)
    with_w = fdot(t_w, ww) + fdot(t_q, wq, NT)
    own_out[...] = lanes([with_q, fdot(with_w, t_w, NT) + fdot(with_q, t_q, NT)], 128)
    stats = products(stack_of(w), stack_of(base, right, w))
    forward_product(rows, 16, matrix, out, stats)


def fourth_sum(cells, rs, keep1, stats1, own1, ag, t_out, l_out):
    total = added(rs)
    stats = tall(total[:, 512:]) * (1.0 / cells)
    grams = [[block_of(stats1, 0)], [block_of(own1, 0), block_of(own1, 1)]]
    lower, t = orthonormal([block_of(stats, 0), block_of(stats, 1)], grams, block_of(stats, 2))
    l_out[...] = lower
    t_out[...] = t
    v = fdot(t, jnp.concatenate([unfolded(total, 16), keep1[16:, :], keep1[:16, :]], axis=0))
    copies(ag, v)


def last_stats(ag3, ag1, lb, ln, t2, left_out, out):
    before, now = lb[...], ln[...]
    left = tdot(t2[...], jnp.concatenate([gathered(ag1), before, now], axis=0))
    left_out[...] = left
    v = gathered(ag3)
    gram = products(stack_of(left, v), stack_of(before, now, left, v))
    copies(out, lanes([gram[:16, :48], gram[16:, :64]], 128))


def finish(stations, rs, base, ag3, lb, ln, left1, ag2, q, right1, t3, l1, l2, l3, rights, left_out, alphas, betas):
    stats = added(rs) * (1.0 / stations)
    grams = [
        [block_of(base, 0)],
        [block_of(base, 1), block_of(base, 2)],
        [block_of(stats, 0), block_of(stats, 1), block_of(stats, 2)],
    ]
    onto = [block_of(stats, 3), block_of(stats, 4), block_of(stats, 5)]
    lower, t = orthonormal(onto, grams, block_of(stats, 6))
    left_out[...] = tdot(t, jnp.concatenate([gathered(ag3), lb[...], ln[...], left1[...]], axis=0))
    rights[0] = right1[...]
    rights[1] = tdot(t3[...], jnp.concatenate([gathered(ag2), q[...], right1[...]], axis=0))
    alphas[0] = l1[...]
    alphas[1] = l3[...]
    betas[0] = l2[...]
    betas[1] = lower


def call(kernel, args, outs, scratch=(), limit=4, where=pltpu.VMEM):
    spec = pl.BlockSpec(memory_space=pltpu.VMEM)
    return pl.pallas_call(
        kernel,
        out_shape=tuple(outs),
        in_specs=[pl.BlockSpec(memory_space=where)] * len(args),
        out_specs=tuple(spec for _ in outs),
        scratch_shapes=list(scratch),
        compiler_params=pltpu.CompilerParams(vmem_limit_bytes=limit * 2**20),
    )(*args)


def f32(*shape):
    return jax.ShapeDtypeStruct(shape, F32)


def exchange(value, axis):
    return lax.all_to_all(value, axis, split_axis=0, concat_axis=0, tiled=True)


def body(station_plane, station_height, cell_plane, cell_depth, cell_density, left_before, left_now, right_before):
    n_s, n_c = left_now.shape[1], right_before.shape[1]
    n_sta, n_cel = lax.axis_size("sta"), lax.axis_size("cel")
    stations, cells = n_s * n_sta, n_c * n_cel
    cp, sp = n_c // n_sta, n_s // n_cel
    small = f32(16, 16)

    inputs = (
        station_plane,
        station_height.reshape(1, n_s),
        cell_plane,
        cell_depth.reshape(1, n_c),
        cell_density.reshape(1, n_c),
        left_before,
        left_now,
        right_before,
    )
    sp_v, sh_v, cp_v, cd_v, rho, lb, ln, q = call(
        fetch,
        inputs,
        [pltpu.VMEM(v.shape, v.dtype) for v in inputs],
        [pltpu.SemaphoreType.DMA((len(inputs),))],
        limit=LARGE,
        where=pltpu.HBM,
    )
    *matrix, rs0, left_rows, stats0 = call(
        first_pass,
        (sp_v, sh_v, cp_v, cd_v, rho, lb, ln),
        (
            *[pltpu.VMEM((n_c // PARTS, n_s), BF16)] * (2 * PARTS),
            f32(n_sta, 32, cp),
            pltpu.VMEM((64, n_s), BF16),
            f32(16, 128),
        ),
        [
            pltpu.VMEM((8, n_s), F32),
            pltpu.VMEM((TILE, 128), F32),
            pltpu.VMEM((TILE, 16), BF16),
            pltpu.VMEM((16, n_s), BF16),
            pltpu.VMEM((TILE, n_s), F32),
        ],
        limit=10,
    )
    ag0, keep0 = call(first_sum, (exchange(rs0, "sta"),), (f32(n_sta, 16, cp), f32(32, cp)))
    ag0 = exchange(ag0, "sta")
    (rs1,) = call(second_pass, (ag0, q, rho, *matrix), (f32(n_cel, 8, 1152),), [pltpu.VMEM((64, n_c), BF16)])
    ag1, keep1, stats1, t1, l1 = call(
        lambda *refs: second_sum(cells, *refs),
        (exchange(rs1, "cel"),),
        (f32(n_cel, 16, sp), f32(32, sp), f32(16, 128), f32(16, 32), small),
    )
    ag1 = exchange(ag1, "cel")
    (rs2,) = call(third_pass, (ag1, left_rows, stats0, rho, *matrix), (f32(n_sta, 32, cp),), [pltpu.VMEM((32, n_s), BF16)])
    ag2, base2, t2, l2 = call(
        lambda *refs: third_sum(stations, *refs),
        (exchange(rs2, "sta"), keep0),
        (f32(n_sta, 16, cp), f32(16, 128), f32(16, 48), small),
    )
    ag2 = exchange(ag2, "sta")
    right1, own1, rs3 = call(
        fourth_pass,
        (ag2, ag0, q, rho, t1, stats1, *matrix),
        (f32(16, n_c), f32(16, 128), f32(n_cel, 8, 640)),
        [pltpu.VMEM((32, n_c), BF16)],
    )
    ag3, t3, l3 = call(
        lambda *refs: fourth_sum(cells, *refs),
        (exchange(rs3, "cel"), keep1, stats1, own1),
        (f32(n_cel, 16, sp), f32(16, 48), small),
    )
    ag3 = exchange(ag3, "cel")
    left1, rs4 = call(last_stats, (ag3, ag1, lb, ln, t2), (f32(16, n_s), f32(n_sta, 16, 128)))
    rights, left2, alphas, betas = call(
        lambda *refs: finish(stations, *refs),
        (exchange(rs4, "sta"), base2, ag3, lb, ln, left1, ag2, q, right1, t3, l1, l2, l3),
        (f32(2, 16, n_c), f32(16, n_s), f32(2, 16, 16), f32(2, 16, 16)),
    )
    return rights, left2, alphas, betas


def solution(mesh):
    in_specs = (
        P(None, "sta"),
        P("sta"),
        P(None, "cel"),
        P("cel"),
        P("cel"),
        P(None, "sta"),
        P(None, "sta"),
        P(None, "cel"),
    )
    out_specs = (P(None, None, "cel"), P(None, "sta"), P(), P())
    return jax.shard_map(body, mesh=mesh, in_specs=in_specs, out_specs=out_specs, check_vma=False)
```

```python
import functools

import jax
import jax.numpy as jnp
from jax import lax
from jax.experimental import pallas as pl
from jax.experimental.pallas import tpu as pltpu
from jax.sharding import PartitionSpec as P

F32 = jnp.float32
BF16 = jnp.bfloat16
HIGH = lax.Precision.HIGHEST
TILE = 256
NN = (((1,), (0,)), ((), ()))
NT = (((1,), (1,)), ((), ()))


def fdot(a, b, dims=NN):
    return lax.dot_general(a, b, dims, precision=HIGH, preferred_element_type=F32)


def bdot(a, b, dims=NN):
    return lax.dot_general(a, b, dims, preferred_element_type=F32)


def halves(x):
    hi = x.astype(BF16)
    lo = (x - hi.astype(F32)).astype(BF16)
    return hi, lo


def lanes(blocks, width):
    used = sum(b.shape[1] for b in blocks)
    rows = blocks[0].shape[0]
    return jnp.concatenate([*blocks, jnp.zeros((rows, width - used), F32)], axis=1)


def block_of(stats, index):
    return stats[:, 16 * index : 16 * index + 16]


def wide(stats):
    return lanes([stats[:8], stats[8:]], 128)


def tall(tile):
    return jnp.concatenate([tile[:, :48], tile[:, 48:96]], axis=0)


def unfolded(message, count):
    return jnp.concatenate([message[:, 256 * k : 256 * k + 256] for k in range(count // 8)], axis=0)


def factor(gram):
    size = gram.shape[0]
    shape = (size, 128)
    row = lax.broadcasted_iota(jnp.int32, shape, 0)
    lane = lax.broadcasted_iota(jnp.int32, shape, 1)
    columns = [jnp.broadcast_to(gram[:, k : k + 1], shape) for k in range(size)]
    inv = jnp.where(lane == row, 1.0, 0.0)
    lower = jnp.zeros(shape, F32)
    for k in range(size):
        pivot = columns[k][k : k + 1, :]
        r = lax.rsqrt(pivot)
        r = r * (1.5 - 0.5 * pivot * r * r)
        column = columns[k] * r
        for j in range(k + 1, size):
            columns[j] = columns[j] - column * column[j : j + 1, :]
        lower = jnp.where((lane == k) & (row >= k), column, lower)
        line = inv[k : k + 1, :] * r
        inv = jnp.where(row == k, line, inv - jnp.where(row > k, column, 0.0) * line)
    return lower[:, :size], inv[:, :size]


def orthonormal(onto, basis, own):
    count = len(onto)
    coef = jnp.concatenate(onto, axis=1)
    lines = []
    for m in range(count):
        line = [*basis[m][:m], 0.5 * basis[m][m]] + [jnp.zeros_like(own)] * (count - 1 - m)
        lines.append(jnp.concatenate(line, axis=1))
    part = fdot(coef, jnp.concatenate(lines, axis=0)) - coef
    gram = own + (fdot(part, coef, NT) + fdot(coef, part, NT))
    lower, inv = factor(gram)
    return lower, jnp.concatenate([inv, -fdot(inv, coef)], axis=1)


def tdot(t, x):
    t_hi, t_lo = halves(t)
    x_hi, x_lo = halves(x)
    size = t.shape[0]
    big = bdot(jnp.concatenate([t_hi, t_lo], axis=0), x_hi)
    return big[:size] + (big[size:] + bdot(t_hi, x_lo))


def added(ref):
    total = ref[0]
    for k in range(1, ref.shape[0]):
        total = total + ref[k]
    return total


def copies(ref, value):
    for k in range(ref.shape[0]):
        ref[k] = value


def gathered(ref):
    return jnp.concatenate([ref[k] for k in range(ref.shape[0])], axis=1)


def stack_of(*values):
    parts = [halves(v) for v in values]
    return jnp.concatenate([p[0] for p in parts] + [p[1] for p in parts], axis=0)


def products(x, y):
    m, k = x.shape[0] // 2, y.shape[0] // 2
    full = bdot(x, y, NT)
    return full[:m, :k] + (full[:m, k:] + full[m:, :k]) + full[m:, k:]


PARTS = 2
LARGE = 62


def pieces(x):
    first = x.astype(BF16).astype(F32)
    second = (x - first).astype(BF16).astype(F32)
    return [first, second, x - first - second]


def fetch(*refs):
    count = len(refs) // 2
    sems = refs[-1]
    moves = [pltpu.make_async_copy(refs[k], refs[count + k], sems.at[k]) for k in range(count)]
    for move in moves:
        move.start()
    for move in moves:
        move.wait()


def first_pass(sp_v, sh_v, cp_v, cd_v, rho_v, lb_v, ln_v, *refs):
    matrix, refs = refs[: 2 * PARTS], refs[2 * PARTS :]
    out, rows, stats_out, sz_v, czb, a_ref, b_ref, square = refs
    n_s, n_c = sp_v.shape[1], cp_v.shape[1]

    sx, sy = sp_v[0:1, :].astype(F32), sp_v[1:2, :].astype(F32)
    sz = sh_v[...].astype(F32) + 0.5
    sz_v[...] = jnp.broadcast_to(sz, sz_v.shape)
    one, zero = jnp.ones_like(sx), jnp.zeros_like(sx)
    b_rows = pieces(sx * sx + sy * sy + sz * sz) + [one, one, one, -2.0 * sx, -2.0 * sy, 2.0 * sz] + [zero] * 7
    b_ref[...] = jnp.concatenate(b_rows, axis=0).astype(BF16)

    rows[...] = stack_of(ln_v[...], lb_v[...])
    gram = products(rows[...], rows[...])
    stats_out[...] = lanes([gram[16:, 16:], gram[:16, 16:], gram[:16, :16]], 128)

    def prepare(c0):
        for half in range(2):
            here = pl.ds(pl.multiple_of(c0 + 128 * half, 128), 128)
            put = slice(128 * half, 128 * half + 128)
            cx, cy = cp_v[0:1, here].astype(F32), cp_v[1:2, here].astype(F32)
            cz = cd_v[0:1, here].astype(F32)
            unit, none = jnp.ones_like(cx), jnp.zeros_like(cx)
            a_rows = [unit, unit, unit] + pieces(cx * cx + cy * cy + cz * cz) + [cx, cy, cz] + [none] * 7
            turned = jnp.transpose(jnp.concatenate(a_rows, axis=0))
            a_ref[put, :] = turned.astype(BF16)
            czb[put, :] = jnp.broadcast_to(turned[:, 8:9], (128, 128))

    def cell_block(part, cb, carry):
        hi_ref, lo_ref = matrix[2 * part], matrix[2 * part + 1]
        g0 = pl.multiple_of(cb * TILE, TILE)
        c0 = pl.multiple_of(part * (n_c // PARTS) + g0, TILE)

        def station_block(sb, inner):
            for half in range(2):
                here = pl.ds(pl.multiple_of(sb * 2 * TILE + half * TILE, TILE), TILE)
                height = sz_v[:, here]
                for r0 in range(0, TILE, 8):
                    dz = height + jnp.concatenate([czb[r0 : r0 + 8, :]] * 2, axis=1)
                    inv = lax.rsqrt(square[r0 : r0 + 8, here])
                    inv2 = inv * inv
                    g = (dz * dz * inv2 - (1.0 / 3.0)) * (inv2 * inv)
                    where = pl.ds(pl.multiple_of(g0 + r0, 8), 8)
                    hi_ref[where, here] = g.astype(BF16)
                    lo_ref[where, here] = (g - hi_ref[where, here].astype(F32)).astype(BF16)
            return inner

        lax.fori_loop(0, n_s // (2 * TILE), station_block, 0)
        prepare(jnp.minimum(c0 + TILE, n_c - TILE))
        total = jnp.zeros((32, TILE), F32)
        for k in range(n_s // TILE):
            own = slice(k * TILE, k * TILE + TILE)
            square[:, own] = bdot(a_ref[...], b_ref[:, own])
            big = bdot(rows[:, own], hi_ref[pl.ds(g0, TILE), own], NT)
            small = bdot(rows[:32, own], lo_ref[pl.ds(g0, TILE), own], NT)
            total = total + (big[:32] + big[32:] + small)
        total = total * (12.0 * rho_v[0:1, pl.ds(c0, TILE)])
        for k in range(2):
            piece = 2 * cb + k + part * (n_c // PARTS // 128)
            out[piece] = total[:, 128 * k : 128 * k + 128]
        return carry

    prepare(0)
    square[...] = bdot(a_ref[...], b_ref[...])
    for part in range(PARTS):
        lax.fori_loop(0, n_c // PARTS // TILE, functools.partial(cell_block, part), 0)


def first_sum(rs, ag, keep):
    total = added(rs)
    keep[...] = total
    copies(ag, total[:16])


def forward_product(rows, count, matrix, out, stats):
    step = 4 * TILE
    size = matrix[0].shape[0]
    tile = wide(stats)

    def station_block(sb, carry):
        s0 = pl.multiple_of(sb * step, step)
        total = jnp.zeros((count, step), F32)
        for part in range(PARTS):
            own = slice(part * size, part * size + size)
            big = bdot(rows[:, own], matrix[2 * part][:, pl.ds(s0, step)])
            small = bdot(rows[:count, own], matrix[2 * part + 1][:, pl.ds(s0, step)])
            total = total + (big[:count] + big[count:] + small)
        for k in range(step // TILE):
            piece = sb * (step // TILE) + k
            for r in range(count // 8):
                out[piece, :, 256 * r : 256 * r + 256] = total[8 * r : 8 * r + 8, TILE * k : TILE * k + TILE]
            out[piece, :, 32 * count :] = tile
        return carry

    lax.fori_loop(0, matrix[0].shape[1] // step, station_block, 0)


def second_pass(ag, q, rho, *refs):
    matrix, (out, rows) = refs[: 2 * PARTS], refs[2 * PARTS :]
    w = gathered(ag)
    base = q[...]
    scale = 12.0 * rho[...]
    rows[...] = stack_of(w * scale, base * scale)
    pair = stack_of(w, base)
    gram = products(pair, pair)
    stats = jnp.concatenate([gram[16:, 16:], gram[:16, 16:], gram[:16, :16]], axis=1)
    forward_product(rows, 32, matrix, out, stats)


def second_sum(cells, rs, ag, keep, stats_out, t_out, l_out):
    total = added(rs)
    rows = unfolded(total, 32)
    stats = tall(total[:, 1024:]) * (1.0 / cells)
    stats_out[...] = lanes([stats], 128)
    lower, t = orthonormal([block_of(stats, 1)], [[block_of(stats, 0)]], block_of(stats, 2))
    l_out[...] = lower
    t_out[...] = t
    v = fdot(t, rows)
    keep[...] = jnp.concatenate([v, rows[16:]], axis=0)
    copies(ag, v)


def third_pass(ag, left_rows, stats0, rho, *refs):
    matrix, (out, rows) = refs[: 2 * PARTS], refs[2 * PARTS :]
    v = gathered(ag)
    rows[...] = stack_of(v)
    gram = products(rows[...], left_rows[...])
    stats = lanes([gram[:, 16:], gram[:, :16], products(rows[...], rows[...]), stats0[:, :48]], 128)

    size = matrix[0].shape[0]
    step = 2 * TILE

    def cell_block(part, cb, carry):
        g0 = pl.multiple_of(cb * step, step)
        c0 = pl.multiple_of(part * size + g0, step)
        big = bdot(rows[...], matrix[2 * part][pl.ds(g0, step), :], NT)
        small = bdot(rows[:16, :], matrix[2 * part + 1][pl.ds(g0, step), :], NT)
        total = (big[:16] + big[16:] + small) * (12.0 * rho[0:1, pl.ds(c0, step)])
        for k in range(step // 128):
            piece = step // 128 * cb + k + part * (size // 128)
            out[piece, :16, :] = total[:, 128 * k : 128 * k + 128]
            out[piece, 16:, :] = stats
        return carry

    for part in range(PARTS):
        lax.fori_loop(0, size // step, functools.partial(cell_block, part), 0)


def third_sum(stations, rs, keep0, ag, base_out, t_out, l_out):
    total = added(rs)
    stats = total[16:] * (1.0 / stations)
    base = stats[:, 48:96]
    base_out[...] = lanes([base], 128)
    grams = [[block_of(base, 0)], [block_of(base, 1), block_of(base, 2)]]
    lower, t = orthonormal([block_of(stats, 0), block_of(stats, 1)], grams, block_of(stats, 2))
    l_out[...] = lower
    t_out[...] = t
    w = fdot(t, jnp.concatenate([total[:16], keep0[16:32, :], keep0[:16, :]], axis=0))
    copies(ag, w)


def fourth_pass(ag2, ag0, q, rho, t1, stats1, *refs):
    matrix, (right_out, own_out, out, rows) = refs[: 2 * PARTS], refs[2 * PARTS :]
    base = q[...]
    right = tdot(t1[...], jnp.concatenate([gathered(ag0), base], axis=0))
    right_out[...] = right
    w = gathered(ag2)
    rows[...] = stack_of(w * (12.0 * rho[...]))
    t_w, t_q = t1[:, :16], t1[:, 16:]
    qq, wq, ww = block_of(stats1, 0), block_of(stats1, 1), block_of(stats1, 2)
    with_q = fdot(t_w, wq) + fdot(t_q, qq)
    with_w = fdot(t_w, ww) + fdot(t_q, wq, NT)
    own_out[...] = lanes([with_q, fdot(with_w, t_w, NT) + fdot(with_q, t_q, NT)], 128)
    stats = products(stack_of(w), stack_of(base, right, w))
    forward_product(rows, 16, matrix, out, stats)


def fourth_sum(cells, rs, keep1, stats1, own1, ag, t_out, l_out):
    total = added(rs)
    stats = tall(total[:, 512:]) * (1.0 / cells)
    grams = [[block_of(stats1, 0)], [block_of(own1, 0), block_of(own1, 1)]]
    lower, t = orthonormal([block_of(stats, 0), block_of(stats, 1)], grams, block_of(stats, 2))
    l_out[...] = lower
    t_out[...] = t
    v = fdot(t, jnp.concatenate([unfolded(total, 16), keep1[16:, :], keep1[:16, :]], axis=0))
    copies(ag, v)


def last_stats(ag3, ag1, lb, ln, t2, left_out, out):
    before, now = lb[...], ln[...]
    left = tdot(t2[...], jnp.concatenate([gathered(ag1), before, now], axis=0))
    left_out[...] = left
    v = gathered(ag3)
    gram = products(stack_of(left, v), stack_of(before, now, left, v))
    copies(out, lanes([gram[:16, :48], gram[16:, :64]], 128))


def finish(stations, rs, base, ag3, lb, ln, left1, ag2, q, right1, t3, l1, l2, l3, rights, left_out, alphas, betas):
    stats = added(rs) * (1.0 / stations)
    grams = [
        [block_of(base, 0)],
        [block_of(base, 1), block_of(base, 2)],
        [block_of(stats, 0), block_of(stats, 1), block_of(stats, 2)],
    ]
    onto = [block_of(stats, 3), block_of(stats, 4), block_of(stats, 5)]
    lower, t = orthonormal(onto, grams, block_of(stats, 6))
    left_out[...] = tdot(t, jnp.concatenate([gathered(ag3), lb[...], ln[...], left1[...]], axis=0))
    rights[0] = right1[...]
    rights[1] = tdot(t3[...], jnp.concatenate([gathered(ag2), q[...], right1[...]], axis=0))
    alphas[0] = l1[...]
    alphas[1] = l3[...]
    betas[0] = l2[...]
    betas[1] = lower


def call(kernel, args, outs, scratch=(), limit=4, where=pltpu.VMEM):
    spec = pl.BlockSpec(memory_space=pltpu.VMEM)
    return pl.pallas_call(
        kernel,
        out_shape=tuple(outs),
        in_specs=[pl.BlockSpec(memory_space=where)] * len(args),
        out_specs=tuple(spec for _ in outs),
        scratch_shapes=list(scratch),
        compiler_params=pltpu.CompilerParams(vmem_limit_bytes=limit * 2**20),
    )(*args)


def f32(*shape):
    return jax.ShapeDtypeStruct(shape, F32)


def exchange(value, axis):
    return lax.all_to_all(value, axis, split_axis=0, concat_axis=0, tiled=True)


def body(station_plane, station_height, cell_plane, cell_depth, cell_density, left_before, left_now, right_before):
    n_s, n_c = left_now.shape[1], right_before.shape[1]
    n_sta, n_cel = lax.axis_size("sta"), lax.axis_size("cel")
    stations, cells = n_s * n_sta, n_c * n_cel
    cp, sp = n_c // n_sta, n_s // n_cel
    small = f32(16, 16)

    inputs = (
        station_plane,
        station_height.reshape(1, n_s),
        cell_plane,
        cell_depth.reshape(1, n_c),
        cell_density.reshape(1, n_c),
        left_before,
        left_now,
        right_before,
    )
    sp_v, sh_v, cp_v, cd_v, rho, lb, ln, q = call(
        fetch,
        inputs,
        [pltpu.VMEM(v.shape, v.dtype) for v in inputs],
        [pltpu.SemaphoreType.DMA((len(inputs),))],
        limit=LARGE,
        where=pltpu.HBM,
    )
    *matrix, rs0, left_rows, stats0 = call(
        first_pass,
        (sp_v, sh_v, cp_v, cd_v, rho, lb, ln),
        (
            *[pltpu.VMEM((n_c // PARTS, n_s), BF16)] * (2 * PARTS),
            f32(n_sta, 32, cp),
            pltpu.VMEM((64, n_s), BF16),
            f32(16, 128),
        ),
        [
            pltpu.VMEM((8, n_s), F32),
            pltpu.VMEM((TILE, 128), F32),
            pltpu.VMEM((TILE, 16), BF16),
            pltpu.VMEM((16, n_s), BF16),
            pltpu.VMEM((TILE, n_s), F32),
        ],
        limit=10,
    )
    ag0, keep0 = call(first_sum, (exchange(rs0, "sta"),), (f32(n_sta, 16, cp), f32(32, cp)))
    ag0 = exchange(ag0, "sta")
    (rs1,) = call(second_pass, (ag0, q, rho, *matrix), (f32(n_cel, 8, 1152),), [pltpu.VMEM((64, n_c), BF16)])
    ag1, keep1, stats1, t1, l1 = call(
        lambda *refs: second_sum(cells, *refs),
        (exchange(rs1, "cel"),),
        (f32(n_cel, 16, sp), f32(32, sp), f32(16, 128), f32(16, 32), small),
    )
    ag1 = exchange(ag1, "cel")
    (rs2,) = call(third_pass, (ag1, left_rows, stats0, rho, *matrix), (f32(n_sta, 32, cp),), [pltpu.VMEM((32, n_s), BF16)])
    ag2, base2, t2, l2 = call(
        lambda *refs: third_sum(stations, *refs),
        (exchange(rs2, "sta"), keep0),
        (f32(n_sta, 16, cp), f32(16, 128), f32(16, 48), small),
    )
    ag2 = exchange(ag2, "sta")
    right1, own1, rs3 = call(
        fourth_pass,
        (ag2, ag0, q, rho, t1, stats1, *matrix),
        (f32(16, n_c), f32(16, 128), f32(n_cel, 8, 640)),
        [pltpu.VMEM((32, n_c), BF16)],
    )
    ag3, t3, l3 = call(
        lambda *refs: fourth_sum(cells, *refs),
        (exchange(rs3, "cel"), keep1, stats1, own1),
        (f32(n_cel, 16, sp), f32(16, 48), small),
    )
    ag3 = exchange(ag3, "cel")
    left1, rs4 = call(last_stats, (ag3, ag1, lb, ln, t2), (f32(16, n_s), f32(n_sta, 16, 128)))
    rights, left2, alphas, betas = call(
        lambda *refs: finish(stations, *refs),
        (exchange(rs4, "sta"), base2, ag3, lb, ln, left1, ag2, q, right1, t3, l1, l2, l3),
        (f32(2, 16, n_c), f32(16, n_s), f32(2, 16, 16), f32(2, 16, 16)),
    )
    return rights, left2, alphas, betas


def solution(mesh):
    in_specs = (
        P(None, "sta"),
        P("sta"),
        P(None, "cel"),
        P("cel"),
        P("cel"),
        P(None, "sta"),
        P(None, "sta"),
        P(None, "cel"),
    )
    out_specs = (P(None, None, "cel"), P(None, "sta"), P(), P())
    return jax.shard_map(body, mesh=mesh, in_specs=in_specs, out_specs=out_specs, check_vma=False)
```

```python
import functools

import jax
import jax.numpy as jnp
from jax import lax
from jax.experimental import pallas as pl
from jax.experimental.pallas import tpu as pltpu
from jax.sharding import PartitionSpec as P

F32 = jnp.float32
BF16 = jnp.bfloat16
HIGH = lax.Precision.HIGHEST
TILE = 256
NN = (((1,), (0,)), ((), ()))
NT = (((1,), (1,)), ((), ()))


def fdot(a, b, dims=NN):
    return lax.dot_general(a, b, dims, precision=HIGH, preferred_element_type=F32)


def bdot(a, b, dims=NN):
    return lax.dot_general(a, b, dims, preferred_element_type=F32)


def halves(x):
    hi = x.astype(BF16)
    lo = (x - hi.astype(F32)).astype(BF16)
    return hi, lo


def lanes(blocks, width):
    used = sum(b.shape[1] for b in blocks)
    rows = blocks[0].shape[0]
    return jnp.concatenate([*blocks, jnp.zeros((rows, width - used), F32)], axis=1)


def block_of(stats, index):
    return stats[:, 16 * index : 16 * index + 16]


def wide(stats):
    return lanes([stats[:8], stats[8:]], 128)


def tall(tile):
    return jnp.concatenate([tile[:, :48], tile[:, 48:96]], axis=0)


def unfolded(message, count):
    return jnp.concatenate([message[:, 256 * k : 256 * k + 256] for k in range(count // 8)], axis=0)


def factor(gram):
    size = gram.shape[0]
    shape = (size, 128)
    row = lax.broadcasted_iota(jnp.int32, shape, 0)
    lane = lax.broadcasted_iota(jnp.int32, shape, 1)
    columns = [jnp.broadcast_to(gram[:, k : k + 1], shape) for k in range(size)]
    inv = jnp.where(lane == row, 1.0, 0.0)
    lower = jnp.zeros(shape, F32)
    for k in range(size):
        pivot = columns[k][k : k + 1, :]
        r = lax.rsqrt(pivot)
        r = r * (1.5 - 0.5 * pivot * r * r)
        column = columns[k] * r
        for j in range(k + 1, size):
            columns[j] = columns[j] - column * column[j : j + 1, :]
        lower = jnp.where((lane == k) & (row >= k), column, lower)
        line = inv[k : k + 1, :] * r
        inv = jnp.where(row == k, line, inv - jnp.where(row > k, column, 0.0) * line)
    return lower[:, :size], inv[:, :size]


def orthonormal(onto, basis, own):
    count = len(onto)
    coef = jnp.concatenate(onto, axis=1)
    lines = []
    for m in range(count):
        line = [*basis[m][:m], 0.5 * basis[m][m]] + [jnp.zeros_like(own)] * (count - 1 - m)
        lines.append(jnp.concatenate(line, axis=1))
    part = fdot(coef, jnp.concatenate(lines, axis=0)) - coef
    gram = own + (fdot(part, coef, NT) + fdot(coef, part, NT))
    lower, inv = factor(gram)
    return lower, jnp.concatenate([inv, -fdot(inv, coef)], axis=1)


def tdot(t, x):
    t_hi, t_lo = halves(t)
    x_hi, x_lo = halves(x)
    size = t.shape[0]
    big = bdot(jnp.concatenate([t_hi, t_lo], axis=0), x_hi)
    return big[:size] + (big[size:] + bdot(t_hi, x_lo))


def added(ref):
    total = ref[0]
    for k in range(1, ref.shape[0]):
        total = total + ref[k]
    return total


def copies(ref, value):
    for k in range(ref.shape[0]):
        ref[k] = value


def gathered(ref):
    return jnp.concatenate([ref[k] for k in range(ref.shape[0])], axis=1)


def stack_of(*values):
    parts = [halves(v) for v in values]
    return jnp.concatenate([p[0] for p in parts] + [p[1] for p in parts], axis=0)


def products(x, y):
    m, k = x.shape[0] // 2, y.shape[0] // 2
    full = bdot(x, y, NT)
    return full[:m, :k] + (full[:m, k:] + full[m:, :k]) + full[m:, k:]


PARTS = 2
LARGE = 62


def pieces(x):
    first = x.astype(BF16).astype(F32)
    second = (x - first).astype(BF16).astype(F32)
    return [first, second, x - first - second]


def fetch(*refs):
    count = len(refs) // 2
    sems = refs[-1]
    moves = [pltpu.make_async_copy(refs[k], refs[count + k], sems.at[k]) for k in range(count)]
    for move in moves:
        move.start()
    for move in moves:
        move.wait()


def first_pass(sp_v, sh_v, cp_v, cd_v, rho_v, lb_v, ln_v, *refs):
    matrix, refs = refs[: 2 * PARTS], refs[2 * PARTS :]
    out, rows, stats_out, sz_v, czb, a_ref, b_ref, square = refs
    n_s, n_c = sp_v.shape[1], cp_v.shape[1]

    sx, sy = sp_v[0:1, :].astype(F32), sp_v[1:2, :].astype(F32)
    sz = sh_v[...].astype(F32) + 0.5
    sz_v[...] = jnp.broadcast_to(sz, sz_v.shape)
    one, zero = jnp.ones_like(sx), jnp.zeros_like(sx)
    b_rows = pieces(sx * sx + sy * sy + sz * sz) + [one, one, one, -2.0 * sx, -2.0 * sy, 2.0 * sz] + [zero] * 7
    b_ref[...] = jnp.concatenate(b_rows, axis=0).astype(BF16)

    rows[...] = stack_of(ln_v[...], lb_v[...])
    gram = products(rows[...], rows[...])
    stats_out[...] = lanes([gram[16:, 16:], gram[:16, 16:], gram[:16, :16]], 128)

    def prepare(c0):
        for half in range(2):
            here = pl.ds(pl.multiple_of(c0 + 128 * half, 128), 128)
            put = slice(128 * half, 128 * half + 128)
            cx, cy = cp_v[0:1, here].astype(F32), cp_v[1:2, here].astype(F32)
            cz = cd_v[0:1, here].astype(F32)
            unit, none = jnp.ones_like(cx), jnp.zeros_like(cx)
            a_rows = [unit, unit, unit] + pieces(cx * cx + cy * cy + cz * cz) + [cx, cy, cz] + [none] * 7
            turned = jnp.transpose(jnp.concatenate(a_rows, axis=0))
            a_ref[put, :] = turned.astype(BF16)
            czb[put, :] = jnp.broadcast_to(turned[:, 8:9], (128, 128))

    def cell_block(part, cb, carry):
        hi_ref, lo_ref = matrix[2 * part], matrix[2 * part + 1]
        g0 = pl.multiple_of(cb * TILE, TILE)
        c0 = pl.multiple_of(part * (n_c // PARTS) + g0, TILE)

        def station_block(sb, inner):
            for half in range(4):
                here = pl.ds(pl.multiple_of(sb * 4 * TILE + half * TILE, TILE), TILE)
                height = sz_v[:, here]
                for r0 in range(0, TILE, 8):
                    dz = height + jnp.concatenate([czb[r0 : r0 + 8, :]] * 2, axis=1)
                    inv = lax.rsqrt(square[r0 : r0 + 8, here])
                    inv2 = inv * inv
                    g = (dz * dz * inv2 - (1.0 / 3.0)) * (inv2 * inv)
                    where = pl.ds(pl.multiple_of(g0 + r0, 8), 8)
                    hi_ref[where, here] = g.astype(BF16)
                    lo_ref[where, here] = (g - hi_ref[where, here].astype(F32)).astype(BF16)
            return inner

        lax.fori_loop(0, n_s // (4 * TILE), station_block, 0)
        prepare(jnp.minimum(c0 + TILE, n_c - TILE))
        total = jnp.zeros((32, TILE), F32)
        for k in range(n_s // TILE):
            own = slice(k * TILE, k * TILE + TILE)
            square[:, own] = bdot(a_ref[...], b_ref[:, own])
            big = bdot(rows[:, own], hi_ref[pl.ds(g0, TILE), own], NT)
            small = bdot(rows[:32, own], lo_ref[pl.ds(g0, TILE), own], NT)
            total = total + (big[:32] + big[32:] + small)
        total = total * (12.0 * rho_v[0:1, pl.ds(c0, TILE)])
        for k in range(2):
            piece = 2 * cb + k + part * (n_c // PARTS // 128)
            out[piece] = total[:, 128 * k : 128 * k + 128]
        return carry

    prepare(0)
    square[...] = bdot(a_ref[...], b_ref[...])
    for part in range(PARTS):
        lax.fori_loop(0, n_c // PARTS // TILE, functools.partial(cell_block, part), 0)


def first_sum(rs, ag, keep):
    total = added(rs)
    keep[...] = total
    copies(ag, total[:16])


def forward_product(rows, count, matrix, out, stats):
    step = 8 * TILE
    size = matrix[0].shape[0]
    tile = wide(stats)

    def station_block(sb, carry):
        s0 = pl.multiple_of(sb * step, step)
        total = jnp.zeros((count, step), F32)
        for part in range(PARTS):
            own = slice(part * size, part * size + size)
            big = bdot(rows[:, own], matrix[2 * part][:, pl.ds(s0, step)])
            small = bdot(rows[:count, own], matrix[2 * part + 1][:, pl.ds(s0, step)])
            total = total + (big[:count] + big[count:] + small)
        for k in range(step // TILE):
            piece = sb * (step // TILE) + k
            for r in range(count // 8):
                out[piece, :, 256 * r : 256 * r + 256] = total[8 * r : 8 * r + 8, TILE * k : TILE * k + TILE]
            out[piece, :, 32 * count :] = tile
        return carry

    lax.fori_loop(0, matrix[0].shape[1] // step, station_block, 0)


def second_pass(ag, q, rho, *refs):
    matrix, (out, rows) = refs[: 2 * PARTS], refs[2 * PARTS :]
    w = gathered(ag)
    base = q[...]
    scale = 12.0 * rho[...]
    rows[...] = stack_of(w * scale, base * scale)
    pair = stack_of(w, base)
    gram = products(pair, pair)
    stats = jnp.concatenate([gram[16:, 16:], gram[:16, 16:], gram[:16, :16]], axis=1)
    forward_product(rows, 32, matrix, out, stats)


def second_sum(cells, rs, ag, keep, stats_out, t_out, l_out):
    total = added(rs)
    rows = unfolded(total, 32)
    stats = tall(total[:, 1024:]) * (1.0 / cells)
    stats_out[...] = lanes([stats], 128)
    lower, t = orthonormal([block_of(stats, 1)], [[block_of(stats, 0)]], block_of(stats, 2))
    l_out[...] = lower
    t_out[...] = t
    v = fdot(t, rows)
    keep[...] = jnp.concatenate([v, rows[16:]], axis=0)
    copies(ag, v)


def third_pass(ag, left_rows, stats0, rho, *refs):
    matrix, (out, rows) = refs[: 2 * PARTS], refs[2 * PARTS :]
    v = gathered(ag)
    rows[...] = stack_of(v)
    gram = products(rows[...], left_rows[...])
    stats = lanes([gram[:, 16:], gram[:, :16], products(rows[...], rows[...]), stats0[:, :48]], 128)

    size = matrix[0].shape[0]
    step = 2 * TILE

    def cell_block(part, cb, carry):
        g0 = pl.multiple_of(cb * step, step)
        c0 = pl.multiple_of(part * size + g0, step)
        big = bdot(rows[...], matrix[2 * part][pl.ds(g0, step), :], NT)
        small = bdot(rows[:16, :], matrix[2 * part + 1][pl.ds(g0, step), :], NT)
        total = (big[:16] + big[16:] + small) * (12.0 * rho[0:1, pl.ds(c0, step)])
        for k in range(step // 128):
            piece = step // 128 * cb + k + part * (size // 128)
            out[piece, :16, :] = total[:, 128 * k : 128 * k + 128]
            out[piece, 16:, :] = stats
        return carry

    for part in range(PARTS):
        lax.fori_loop(0, size // step, functools.partial(cell_block, part), 0)


def third_sum(stations, rs, keep0, ag, base_out, t_out, l_out):
    total = added(rs)
    stats = total[16:] * (1.0 / stations)
    base = stats[:, 48:96]
    base_out[...] = lanes([base], 128)
    grams = [[block_of(base, 0)], [block_of(base, 1), block_of(base, 2)]]
    lower, t = orthonormal([block_of(stats, 0), block_of(stats, 1)], grams, block_of(stats, 2))
    l_out[...] = lower
    t_out[...] = t
    w = fdot(t, jnp.concatenate([total[:16], keep0[16:32, :], keep0[:16, :]], axis=0))
    copies(ag, w)


def fourth_pass(ag2, ag0, q, rho, t1, stats1, *refs):
    matrix, (right_out, own_out, out, rows) = refs[: 2 * PARTS], refs[2 * PARTS :]
    base = q[...]
    right = tdot(t1[...], jnp.concatenate([gathered(ag0), base], axis=0))
    right_out[...] = right
    w = gathered(ag2)
    rows[...] = stack_of(w * (12.0 * rho[...]))
    t_w, t_q = t1[:, :16], t1[:, 16:]
    qq, wq, ww = block_of(stats1, 0), block_of(stats1, 1), block_of(stats1, 2)
    with_q = fdot(t_w, wq) + fdot(t_q, qq)
    with_w = fdot(t_w, ww) + fdot(t_q, wq, NT)
    own_out[...] = lanes([with_q, fdot(with_w, t_w, NT) + fdot(with_q, t_q, NT)], 128)
    stats = products(stack_of(w), stack_of(base, right, w))
    forward_product(rows, 16, matrix, out, stats)


def fourth_sum(cells, rs, keep1, stats1, own1, ag, t_out, l_out):
    total = added(rs)
    stats = tall(total[:, 512:]) * (1.0 / cells)
    grams = [[block_of(stats1, 0)], [block_of(own1, 0), block_of(own1, 1)]]
    lower, t = orthonormal([block_of(stats, 0), block_of(stats, 1)], grams, block_of(stats, 2))
    l_out[...] = lower
    t_out[...] = t
    v = fdot(t, jnp.concatenate([unfolded(total, 16), keep1[16:, :], keep1[:16, :]], axis=0))
    copies(ag, v)


def last_stats(ag3, ag1, lb, ln, t2, left_out, out):
    before, now = lb[...], ln[...]
    left = tdot(t2[...], jnp.concatenate([gathered(ag1), before, now], axis=0))
    left_out[...] = left
    v = gathered(ag3)
    gram = products(stack_of(left, v), stack_of(before, now, left, v))
    copies(out, lanes([gram[:16, :48], gram[16:, :64]], 128))


def finish(stations, rs, base, ag3, lb, ln, left1, ag2, q, right1, t3, l1, l2, l3, rights, left_out, alphas, betas):
    stats = added(rs) * (1.0 / stations)
    grams = [
        [block_of(base, 0)],
        [block_of(base, 1), block_of(base, 2)],
        [block_of(stats, 0), block_of(stats, 1), block_of(stats, 2)],
    ]
    onto = [block_of(stats, 3), block_of(stats, 4), block_of(stats, 5)]
    lower, t = orthonormal(onto, grams, block_of(stats, 6))
    left_out[...] = tdot(t, jnp.concatenate([gathered(ag3), lb[...], ln[...], left1[...]], axis=0))
    rights[0] = right1[...]
    rights[1] = tdot(t3[...], jnp.concatenate([gathered(ag2), q[...], right1[...]], axis=0))
    alphas[0] = l1[...]
    alphas[1] = l3[...]
    betas[0] = l2[...]
    betas[1] = lower


def call(kernel, args, outs, scratch=(), limit=4, where=pltpu.VMEM):
    spec = pl.BlockSpec(memory_space=pltpu.VMEM)
    return pl.pallas_call(
        kernel,
        out_shape=tuple(outs),
        in_specs=[pl.BlockSpec(memory_space=where)] * len(args),
        out_specs=tuple(spec for _ in outs),
        scratch_shapes=list(scratch),
        compiler_params=pltpu.CompilerParams(vmem_limit_bytes=limit * 2**20),
    )(*args)


def f32(*shape):
    return jax.ShapeDtypeStruct(shape, F32)


def exchange(value, axis):
    return lax.all_to_all(value, axis, split_axis=0, concat_axis=0, tiled=True)


def body(station_plane, station_height, cell_plane, cell_depth, cell_density, left_before, left_now, right_before):
    n_s, n_c = left_now.shape[1], right_before.shape[1]
    n_sta, n_cel = lax.axis_size("sta"), lax.axis_size("cel")
    stations, cells = n_s * n_sta, n_c * n_cel
    cp, sp = n_c // n_sta, n_s // n_cel
    small = f32(16, 16)

    inputs = (
        station_plane,
        station_height.reshape(1, n_s),
        cell_plane,
        cell_depth.reshape(1, n_c),
        cell_density.reshape(1, n_c),
        left_before,
        left_now,
        right_before,
    )
    sp_v, sh_v, cp_v, cd_v, rho, lb, ln, q = call(
        fetch,
        inputs,
        [pltpu.VMEM(v.shape, v.dtype) for v in inputs],
        [pltpu.SemaphoreType.DMA((len(inputs),))],
        limit=LARGE,
        where=pltpu.HBM,
    )
    *matrix, rs0, left_rows, stats0 = call(
        first_pass,
        (sp_v, sh_v, cp_v, cd_v, rho, lb, ln),
        (
            *[pltpu.VMEM((n_c // PARTS, n_s), BF16)] * (2 * PARTS),
            f32(n_sta, 32, cp),
            pltpu.VMEM((64, n_s), BF16),
            f32(16, 128),
        ),
        [
            pltpu.VMEM((8, n_s), F32),
            pltpu.VMEM((TILE, 128), F32),
            pltpu.VMEM((TILE, 16), BF16),
            pltpu.VMEM((16, n_s), BF16),
            pltpu.VMEM((TILE, n_s), F32),
        ],
        limit=10,
    )
    ag0, keep0 = call(first_sum, (exchange(rs0, "sta"),), (f32(n_sta, 16, cp), f32(32, cp)))
    ag0 = exchange(ag0, "sta")
    (rs1,) = call(second_pass, (ag0, q, rho, *matrix), (f32(n_cel, 8, 1152),), [pltpu.VMEM((64, n_c), BF16)])
    ag1, keep1, stats1, t1, l1 = call(
        lambda *refs: second_sum(cells, *refs),
        (exchange(rs1, "cel"),),
        (f32(n_cel, 16, sp), f32(32, sp), f32(16, 128), f32(16, 32), small),
    )
    ag1 = exchange(ag1, "cel")
    (rs2,) = call(third_pass, (ag1, left_rows, stats0, rho, *matrix), (f32(n_sta, 32, cp),), [pltpu.VMEM((32, n_s), BF16)])
    ag2, base2, t2, l2 = call(
        lambda *refs: third_sum(stations, *refs),
        (exchange(rs2, "sta"), keep0),
        (f32(n_sta, 16, cp), f32(16, 128), f32(16, 48), small),
    )
    ag2 = exchange(ag2, "sta")
    right1, own1, rs3 = call(
        fourth_pass,
        (ag2, ag0, q, rho, t1, stats1, *matrix),
        (f32(16, n_c), f32(16, 128), f32(n_cel, 8, 640)),
        [pltpu.VMEM((32, n_c), BF16)],
    )
    ag3, t3, l3 = call(
        lambda *refs: fourth_sum(cells, *refs),
        (exchange(rs3, "cel"), keep1, stats1, own1),
        (f32(n_cel, 16, sp), f32(16, 48), small),
    )
    ag3 = exchange(ag3, "cel")
    left1, rs4 = call(last_stats, (ag3, ag1, lb, ln, t2), (f32(16, n_s), f32(n_sta, 16, 128)))
    rights, left2, alphas, betas = call(
        lambda *refs: finish(stations, *refs),
        (exchange(rs4, "sta"), base2, ag3, lb, ln, left1, ag2, q, right1, t3, l1, l2, l3),
        (f32(2, 16, n_c), f32(16, n_s), f32(2, 16, 16), f32(2, 16, 16)),
    )
    return rights, left2, alphas, betas


def solution(mesh):
    in_specs = (
        P(None, "sta"),
        P("sta"),
        P(None, "cel"),
        P("cel"),
        P("cel"),
        P(None, "sta"),
        P(None, "sta"),
        P(None, "cel"),
    )
    out_specs = (P(None, None, "cel"), P(None, "sta"), P(), P())
    return jax.shard_map(body, mesh=mesh, in_specs=in_specs, out_specs=out_specs, check_vma=False)
```
